32 devices in a mesh: row: 8 (over z, x), col: 4 (over y, core).
Axes of the slice: x: 2, y: 2, z: 4, core: 2. Of those that a mesh axis runs over, the one named last changes fastest.
Arguments:
- points: float32 [3, 4096], P(None, ('row', 'col')), may hold values from 0 to 10, as said below
- weights: float32 [4096], P(('row', 'col')), may hold values from 0.5 to 4
- far_blocks: int32 [8, 8], P('row', 'col'), may hold values from 0 to 7, as said below
- row_pivots: int32 [8, 8, 2, 64], P('row', 'col'), may hold values from 0 to 511
- col_pivots: int32 [8, 8, 2, 64], P('row', 'col'), may hold values from 0 to 511
Outputs:
- factors_v: bfloat16 [8, 1024, 512], P('row', 'col')
- basis_q: bfloat16 [8, 1024, 512], P('row', None, 'col')
- tri_factor: float32 [8, 1024, 1024], P('row')
The draws below stay inside these ranges and needn't reach their ends.
Inputs may be any that keep to these rules, and one draw needn't show every extreme that they name: `points`: the panels of cluster c lie in the unit box whose lowest corner is 3 * (c % 4, (c // 4) % 4, c // 16). `far_blocks`: for every slot, the partners of the 8 clusters form a single cycle through all clusters: no cluster is its own partner, and each cluster is the partner of exactly one cluster in each slot.
All inputs are finite; a program needn't handle non-finite values.
Results may differ from the reference program's by a relative error of at most 0.007.
The reference program's roundings to bfloat16 on the way count: a program that leaves them out, or rounds other values in their place, can miss the bound.
Values may be sent and summed in bfloat16 or wider, within the bound.
No kernel may reach another device: no remote copies, remote signals or barrier semaphores. Data moves between devices by JAX's collectives and lax.ppermute only.
A program may use at most 128 MiB of HBM per device.

```python
import math
import jax
import jax.numpy as jnp
from jax import lax

M = 512
R = 64
ROUNDS = 2
CLUSTERS = 8
SLOTS = 8
PANELS = 4096
BASIS = 1024


def draw_points(key, part):
    cluster = jnp.arange(PANELS, dtype=jnp.int32) // M
    corner = 3.0 * jnp.stack([cluster % 4, cluster // 4 % 4, cluster // 16]).astype(jnp.float32)
    offset = jax.random.uniform(jax.random.fold_in(key, 11), (3, PANELS), jnp.float32)
    return corner + offset


def draw_far_blocks(key, part):

    def one_slot(slot):
        order = jax.random.permutation(jax.random.fold_in(key, 100 + slot), CLUSTERS)
        place = jnp.argsort(order)
        return order[(place + 1) % CLUSTERS].astype(jnp.int32)
    return jax.vmap(one_slot, out_axes=1)(jnp.arange(SLOTS, dtype=jnp.int32))


def place_ends(entries, own_key, low, largest):
    longest = entries.shape.index(max(entries.shape))
    spots = []
    for shift in (0, 1):
        where = [jax.random.randint(jax.random.fold_in(own_key, axis), (), 0, length) for axis, length in enumerate(entries.shape)]
        where[longest] = (where[longest] + shift) % entries.shape[longest]
        spots.append(tuple(where))
    return entries.at[spots[0]].set(low).at[spots[1]].set(largest)


def steps_of(stream_key, dims, cuts, low, high):
    def one(axis_at, shards_of):
        heights = jax.random.uniform(jax.random.fold_in(jax.random.fold_in(stream_key, 6), axis_at), (shards_of,), jnp.float32, low / len(cuts), high / len(cuts))
        return jnp.repeat(jnp.exp(heights), dims[axis_at] // shards_of).reshape((-1,) + (1,) * (len(dims) - axis_at - 1))

    gain = one(*cuts[0])
    for cut in cuts[1:]:
        gain = gain * one(*cut)
    return gain


def setup_inputs(seed: int = 0) -> dict:
    keys = jax.random.split(jax.random.key(seed), 6)
    return {
        "points": draw_points(jax.random.fold_in(keys[5], 71), 0),
        "weights": jnp.clip(jnp.exp(math.log(4.0) - 2.0794415 * jax.random.uniform(keys[1], (PANELS,), jnp.float32) ** steps_of(keys[1], (PANELS,), ((0, 32),), -0.2, 0.2)), 0.5, 4.0),
        "far_blocks": draw_far_blocks(jax.random.fold_in(keys[5], 71), 0),
        "row_pivots": place_ends(jax.random.randint(keys[3], (CLUSTERS, SLOTS, ROUNDS, R), 0, M), jax.random.fold_in(keys[3], 1), 0, M - 1).astype(jnp.int32),
        "col_pivots": place_ends(jax.random.randint(keys[4], (CLUSTERS, SLOTS, ROUNDS, R), 0, M), jax.random.fold_in(keys[4], 1), 0, M - 1).astype(jnp.int32),
    }


wave_number = 8.0

def helmholtz_kernel(sources, targets):
    delta_x = sources[0][:, None] - targets[0][None, :]
    delta_y = sources[1][:, None] - targets[1][None, :]
    delta_z = sources[2][:, None] - targets[2][None, :]
    distance = jnp.sqrt(delta_x * delta_x + delta_y * delta_y + delta_z * delta_z)
    return sources[3][:, None] * targets[3][None, :] * jnp.cos(wave_number * distance) / distance

def solve_lower(lower_factor, rhs, transposed):
    return lax.linalg.triangular_solve(lower_factor, rhs, left_side=True, lower=True, transpose_a=transposed)

def cross_block(own_points, partner_points, row_piv, col_piv):
    rank = row_piv.shape[1]
    left_list = []
    right_list = []
    for counter in range(row_piv.shape[0]):
        own_pivot = jnp.take(own_points, row_piv[counter], axis=1)
        far_pivot = jnp.take(partner_points, col_piv[counter], axis=1)
        col_panel = helmholtz_kernel(far_pivot, own_points)
        row_panel = helmholtz_kernel(own_pivot, partner_points)
        for left_old, right_old in zip(left_list, right_list):
            col_panel = col_panel - jnp.dot(jnp.take(right_old, col_piv[counter], axis=1).T.astype(jnp.float32), left_old.astype(jnp.float32), preferred_element_type=jnp.float32)
            row_panel = row_panel - jnp.dot(jnp.take(left_old, row_piv[counter], axis=1).T.astype(jnp.float32), right_old.astype(jnp.float32), preferred_element_type=jnp.float32)
        pivot_t = jnp.take(col_panel, row_piv[counter], axis=1)
        normal = jnp.dot(pivot_t.astype(jnp.float32), pivot_t.T.astype(jnp.float32), precision=lax.Precision.HIGHEST, preferred_element_type=jnp.float32)
        shift = jnp.sum(pivot_t * pivot_t) / rank + 1e-06
        normal = normal + shift * jnp.eye(rank, dtype=jnp.float32)
        lower_factor = jnp.linalg.cholesky(normal)
        coupling = solve_lower(lower_factor, solve_lower(lower_factor, pivot_t, False), True)
        right_new = jnp.dot(coupling.astype(jnp.float32), row_panel.astype(jnp.float32), precision=lax.Precision.HIGHEST, preferred_element_type=jnp.float32)
        left_list.append(col_panel.astype(jnp.bfloat16))
        right_list.append(right_new.astype(jnp.bfloat16))
    return (jnp.concatenate(left_list, 0), jnp.concatenate(right_list, 0))

def cluster_basis(gram, factor_rows):
    columns = gram.shape[0]
    shift = jnp.trace(gram) / columns + 1e-06
    lower_factor = jnp.linalg.cholesky(gram + shift * jnp.eye(columns, dtype=jnp.float32))
    basis = solve_lower(lower_factor, factor_rows.astype(jnp.float32), False)
    return (lower_factor, basis.astype(jnp.bfloat16))

def reference(points, weights, far_blocks, row_pivots, col_pivots):
    panel_data = jnp.concatenate([points, weights[None, :]], 0)

    def cluster_work(inputs):
        cluster, blocks, row_piv, col_piv = inputs
        own_points = lax.dynamic_slice_in_dim(panel_data, (cluster * M).astype(jnp.int32), M, 1)

        def slot_work(slot_inputs):
            partner, slot_rows, slot_cols = slot_inputs
            partner_points = lax.dynamic_slice_in_dim(panel_data, (partner * M).astype(jnp.int32), M, 1)
            return cross_block(own_points, partner_points, slot_rows, slot_cols)
        lefts, rights = lax.map(slot_work, (blocks, row_piv, col_piv))
        ucat = lefts.reshape(BASIS, M)
        right_all = rights.reshape(BASIS, M)
        gram = lax.dot_general(ucat.astype(jnp.float32), ucat.astype(jnp.float32), (((1,), (1,)), ((), ())), preferred_element_type=jnp.float32) / M
        lower_factor, basis = cluster_basis(gram, ucat)
        return (right_all, basis, lower_factor)
    factors_v, basis_q, tri_factor = lax.map(cluster_work, (jnp.arange(CLUSTERS, dtype=jnp.int32), far_blocks, row_pivots, col_pivots))
    return (factors_v, basis_q, tri_factor)
```

```python
import functools
import math

import jax
import jax.numpy as jnp
from jax import lax
from jax.experimental import pallas as pl
from jax.experimental.pallas import tpu as pltpu
from jax.sharding import PartitionSpec as P

f32, bf16 = jnp.float32, jnp.bfloat16
LANES, SUB = 128, 8

WAVE_NUMBER = 8.0
SINE = [(-1.0) ** k * (2.0 * math.pi) ** (2 * k + 1) / math.factorial(2 * k + 1) for k in range(7)]
NN = (((1,), (0,)), ((), ()))
NT = (((1,), (1,)), ((), ()))
TN = (((0,), (0,)), ((), ()))


def dot(a, b, dims):
    return lax.dot_general(a, b, dims, preferred_element_type=f32)


def split(x):
    hi = x.astype(bf16)
    return hi, (x - hi.astype(f32)).astype(bf16)


def dot3(a, b, dims):
    ah, al = a if isinstance(a, tuple) else split(a)
    bh, bl = b if isinstance(b, tuple) else split(b)
    return dot(ah, bh, dims) + (dot(al, bh, dims) + dot(ah, bl, dims))


def row_bcast(x, j):
    return jnp.broadcast_to(x[j : j + 1, :], x.shape)


def eliminate(parts, groups):
    mats = parts[0]
    lane_shape = (SUB, LANES)
    sub = lax.broadcasted_iota(jnp.int32, lane_shape, 0)
    for g in range(groups):
        panel = {
            (i, t): jnp.broadcast_to(mats[i][:, SUB * g + t : SUB * g + t + 1], lane_shape)
            for i in range(g, groups)
            for t in range(SUB)
        }
        for j in range(SUB):
            scale = lax.rsqrt(row_bcast(panel[g, j], j))
            rows = [row_bcast(p[g], j) * scale for p in parts]
            ahead = {t: row_bcast(panel[g, t], j) * scale for t in range(j + 1, SUB)}
            for i in range(g, groups):
                m = panel[i, j] * scale
                if i == g:
                    m = jnp.where(sub > j, m, 0.0)
                for p, row in zip(parts, rows):
                    new = p[i] - m * row
                    p[i] = jnp.where(sub == j, row, new) if i == g else new
                for t, head in ahead.items():
                    panel[i, t] = panel[i, t] - m * head


def chol_kernel(ucat_ref, basis_ref, tri_ref, a_ref, y_ref, x_ref, pa_ref, pb_ref, sems):
    n, inner = ucat_ref.shape
    blk = LANES
    nb = n // blk
    col = lax.axis_index("col")
    own = pl.ds(pl.multiple_of(col * blk, blk), blk)
    y_ref[...] = ucat_ref[:, own].astype(f32)
    squares = jnp.zeros((SUB, inner), f32)
    for i in range(0, n, 128):
        rows = ucat_ref[i : i + 128, :]
        top = rows.astype(f32)
        squares = squares + jnp.sum((top * top).reshape(16, SUB, inner), axis=0)
        a_ref[i : i + 128, 0 : i + 128] = dot(rows, ucat_ref[0 : i + 128, :], NT) * (1.0 / inner)
    shift = jnp.sum(squares) * (1.0 / (inner * n)) + 1e-06
    eye = lax.broadcasted_iota(jnp.int32, (blk, blk), 0) == lax.broadcasted_iota(
        jnp.int32, (blk, blk), 1
    )

    def copy_out(b):
        strip = pl.ds(pl.multiple_of(b * blk, blk), blk)
        return pltpu.make_async_copy(a_ref.at[:, strip], tri_ref.at[0, :, strip], sems.at[b])

    def block(b, carry):
        here = pl.ds(pl.multiple_of(b * blk, blk), blk)
        d = a_ref[here, here] + jnp.where(eye, shift, 0.0)
        mats = [d[SUB * i : SUB * (i + 1), :] for i in range(blk // SUB)]
        ident = jnp.where(eye, 1.0, 0.0).astype(f32)
        inv = [ident[SUB * i : SUB * (i + 1), :] for i in range(blk // SUB)]
        eliminate([mats, inv], blk // SUB)
        factor_t = jnp.concatenate(mats, 0)
        upper = lax.broadcasted_iota(jnp.int32, (blk, blk), 0) <= lax.broadcasted_iota(
            jnp.int32, (blk, blk), 1
        )
        a_ref[here, here] = jnp.where(upper, factor_t, 0.0).T
        x = jnp.concatenate(inv, 0)
        xs = split(x)
        yb = dot3(xs, y_ref[here, :], NN)
        basis_ref[0, here, :] = yb.astype(bf16)
        ys = split(yb)

        for k in range(nb):

            @pl.when(b == k)
            def _():
                r0 = (k + 1) * blk
                strip = slice(k * blk, r0)
                if k:
                    a_ref[0 : k * blk, strip] = jnp.zeros((k * blk, blk), f32)
                if r0 < n:
                    low = dot3(a_ref[r0:, strip], xs, NT)
                    a_ref[r0:, strip] = low
                    lh, ll = split(low)
                    pa_ref[r0:, 0:blk] = lh
                    pa_ref[r0:, blk : 2 * blk] = ll
                    pa_ref[r0:, 2 * blk :] = lh
                    pb_ref[r0:, 0:blk] = lh
                    pb_ref[r0:, blk : 2 * blk] = lh
                    pb_ref[r0:, 2 * blk :] = ll
                    for c in range(r0, n, 2 * blk):
                        w = min(2 * blk, n - c)
                        a_ref[c:, c : c + w] -= dot(pa_ref[c:, :], pb_ref[c : c + w, :], NT)
                    y_ref[r0:, :] -= dot3((lh, ll), ys, NN)

        copy_out(b).start()
        return carry

    lax.fori_loop(0, nb, block, 0)
    for b in range(nb):
        copy_out(b).wait()


def factor(ucat, part):
    n, inner = ucat.shape
    vmem = pl.BlockSpec(memory_space=pltpu.VMEM)
    return pl.pallas_call(
        chol_kernel,
        out_shape=(
            jax.ShapeDtypeStruct((1, n, part), bf16),
            jax.ShapeDtypeStruct((1, n, n), f32),
        ),
        in_specs=[vmem],
        out_specs=(vmem, pl.BlockSpec(memory_space=pl.ANY)),
        scratch_shapes=[
            pltpu.VMEM((n, n), f32),
            pltpu.VMEM((n, part), f32),
            pltpu.VMEM((LANES, LANES), f32),
            pltpu.VMEM((n, 3 * LANES), bf16),
            pltpu.VMEM((n, 3 * LANES), bf16),
            pltpu.SemaphoreType.DMA((n // LANES,)),
        ],
        compiler_params=pltpu.CompilerParams(vmem_limit_bytes=48 << 20),
        name="factor",
    )(ucat)


def wave(a, b):
    dx, dy, dz = a[0] - b[0], a[1] - b[1], a[2] - b[2]
    square = dx * dx + dy * dy + dz * dz
    inverse = lax.rsqrt(square)
    turns = square * inverse * (WAVE_NUMBER / (2.0 * math.pi))
    rest = jnp.abs(turns - jnp.floor(turns + 0.5))
    x = 0.25 - rest
    xx = x * x
    poly = SINE[-1]
    for c in SINE[-2::-1]:
        poly = poly * xx + c
    return a[3] * b[3] * (poly * x * inverse)


def shifted_inverse(tops):
    rank = tops[0].shape[0]
    groups = rank // SUB
    r = lax.broadcasted_iota(jnp.int32, (rank, rank), 0)
    c = lax.broadcasted_iota(jnp.int32, (rank, rank), 1)
    all_rows = []
    for top in tops:
        s = split(top)
        shift = jnp.sum(top * top) * (1.0 / rank) + 1e-06
        normal = dot3(s, s, NT) + jnp.where(r == c, shift, 0.0)
        both = jnp.concatenate([normal, jnp.where(r == c, 1.0, 0.0).astype(f32)], 1)
        all_rows.append([both[SUB * i : SUB * (i + 1), :] for i in range(groups)])
    eliminate_many(all_rows, groups)
    return [jnp.concatenate(rows, 0)[:, rank:] for rows in all_rows]


def eliminate_many(mats, groups):
    for m in mats:
        eliminate([m], groups)


def cross_kernel(rank, far_ref, tile_ref, ucat_ref, right_ref, pts_ref, ij_ref, ijt_ref, c_ref, v_ref):
    devices = tile_ref.shape[0]
    cols = lax.axis_size("col")
    clusters = devices // cols
    size = cols * LANES
    local = far_ref.shape[1]
    slots = cols * local
    row, col = lax.axis_index("row"), lax.axis_index("col")

    for k in range(clusters):
        p = jnp.concatenate([tile_ref[k * cols + c, 0:4, :] for c in range(cols)], 1)
        hi, mid = split(p)
        lo = (p - hi.astype(f32) - mid.astype(f32)).astype(bf16)
        zero = jnp.zeros((4, size), bf16)
        pts_ref[16 * k : 16 * k + 16, :] = jnp.concatenate([hi, mid, lo, zero], 0)

    spots = lax.broadcasted_iota(jnp.int32, (size, LANES), 0)
    of = lax.broadcasted_iota(jnp.int32, (clusters, 16, LANES), 0)
    for c in range(cols):
        for s in range(local):
            found = []
            for kind in range(2):
                panel = tile_ref[row * cols + c, 4 + kind * local + s : 5 + kind * local + s, :].astype(jnp.int32)
                where = panel // size
                hot = jnp.where(spots == panel - where * size, 1.0, 0.0).astype(bf16)
                got = dot(pts_ref[...], hot, NN).reshape(clusters, 16, LANES)
                got = jnp.sum(jnp.where(of == where[None], got, 0.0), axis=0)
                found.append(got[0:4] + got[4:8] + got[8:12])
            at = 8 * (c * local + s)
            ij_ref[at : at + 8, :] = jnp.concatenate(found, 0)
    ijt_ref[...] = jnp.concatenate([ij_ref[...], jnp.zeros((LANES - 8 * slots, LANES), f32)], 0).T

    own = jnp.concatenate([tile_ref[row * cols + c, 0:4, :] for c in range(cols)], 1)
    own = [own[i : i + 1, :] for i in range(4)]

    def as_rows(slot, kind, k):
        at = 8 * slot + 4 * kind
        return [ij_ref[at + i : at + i + 1, k * rank : (k + 1) * rank] for i in range(4)]

    def as_columns(slot, kind, k):
        at = 8 * slot + 4 * kind
        return [ijt_ref[k * rank : (k + 1) * rank, at + i : at + i + 1] for i in range(4)]

    group = 4
    for first in range(0, slots, group):
        tops = [wave(as_columns(s, 1, 0), as_rows(s, 0, 0)) for s in range(first, first + group)]
        lowers = shifted_inverse(tops)
        for s, top, lower in zip(range(first, first + group), tops, lowers):
            low = split(lower)
            half = dot3(low, split(top), NN)
            coupling = dot3(low, split(half), TN)
            c_ref[s] = coupling
            v_t = dot3(split(wave(as_columns(s, 1, 1), as_rows(s, 0, 0))), split(coupling), NT).astype(bf16)
            v_ref[s] = v_t
            at = s * 2 * rank
            u0 = wave(as_columns(s, 1, 0), own).astype(bf16)
            ucat_ref[at : at + rank, :] = u0
            u1 = wave(as_columns(s, 1, 1), own) - dot(v_t, u0, NN)
            ucat_ref[at + rank : at + 2 * rank, :] = u1.astype(bf16)

    tops, rest = [], []
    for s in range(local):
        slot = col * local + s
        rows = ij_ref[pl.ds(pl.multiple_of(8 * slot, 8), 8), :]
        columns = rows.T
        i_row = [[rows[q : q + 1, k * rank : (k + 1) * rank] for q in range(4)] for k in range(2)]
        j_row = [[rows[4 + q : 5 + q, k * rank : (k + 1) * rank] for q in range(4)] for k in range(2)]
        i_col = [[columns[k * rank : (k + 1) * rank, q : q + 1] for q in range(4)] for k in range(2)]
        j_col = [[columns[k * rank : (k + 1) * rank, 4 + q : 5 + q] for q in range(4)] for k in range(2)]
        far = far_ref[0, s]
        there = jnp.concatenate([tile_ref[far * cols + c, 0:4, :] for c in range(cols)], 1)
        there = [there[q : q + 1, :] for q in range(4)]
        v0 = dot3(split(c_ref[slot]), split(wave(i_col[0], there)), NN).astype(bf16)
        at = s * 2 * rank
        right_ref[0, at : at + rank, :] = v0
        u_t = wave(i_col[1], j_row[0]).astype(bf16)
        row_panel = wave(i_col[1], there) - dot(u_t, v0, NN)
        u_i = wave(j_col[0], i_row[1]).astype(bf16)
        tops.append(wave(j_col[1], i_row[1]) - dot(v_ref[slot], u_i, NN))
        rest.append(row_panel)
    lowers = shifted_inverse(tops)
    for s in range(local):
        low = split(lowers[s])
        coupling = dot3(low, split(dot3(low, split(tops[s]), NN)), TN)
        at = (2 * s + 1) * rank
        right_ref[0, at : at + rank, :] = dot3(split(coupling), split(rest[s]), NN).astype(bf16)


def cross(far_blocks, tiles, rank, cols):
    local = far_blocks.shape[1]
    slots = cols * local
    clusters = tiles.shape[0] // cols
    size = cols * LANES
    vmem = pl.BlockSpec(memory_space=pltpu.VMEM)
    return pl.pallas_call(
        functools.partial(cross_kernel, rank),
        out_shape=(
            jax.ShapeDtypeStruct((slots * 2 * rank, size), bf16),
            jax.ShapeDtypeStruct((1, local * 2 * rank, size), bf16),
        ),
        in_specs=[pl.BlockSpec(memory_space=pltpu.SMEM), vmem],
        out_specs=(vmem, vmem),
        scratch_shapes=[
            pltpu.VMEM((16 * clusters, size), bf16),
            pltpu.VMEM((8 * slots, LANES), f32),
            pltpu.VMEM((LANES, LANES), f32),
            pltpu.VMEM((slots, rank, rank), f32),
            pltpu.VMEM((slots, rank, rank), bf16),
        ],
        compiler_params=pltpu.CompilerParams(vmem_limit_bytes=48 << 20),
        name="cross",
    )(far_blocks, tiles)


def per_device(points, weights, far_blocks, row_pivots, col_pivots):
    part = points.shape[1]
    cols = lax.axis_size("col")
    size = part * cols
    rank = row_pivots.shape[3]
    own = row_pivots[0] + lax.axis_index("row") * size
    far = col_pivots[0] + far_blocks[0][:, None, None] * size
    tile = jnp.concatenate(
        [points, weights[None], own.reshape(-1, part).astype(f32), far.reshape(-1, part).astype(f32)], 0
    )
    count = lax.axis_size("row") * cols
    tiles = lax.all_to_all(
        jnp.broadcast_to(tile[None], (count,) + tile.shape), ("row", "col"), split_axis=0, concat_axis=0, tiled=True
    )
    ucat, factors_v = cross(far_blocks, tiles, rank, cols)
    basis, lower = factor(ucat, part)
    return factors_v, basis, lower


def solution(mesh):
    return jax.shard_map(
        per_device,
        mesh=mesh,
        in_specs=(
            P(None, ("row", "col")),
            P(("row", "col")),
            P("row", "col"),
            P("row", "col", None, None),
            P("row", "col", None, None),
        ),
        out_specs=(P("row", "col", None), P("row", None, "col"), P("row", None, None)),
        check_vma=False,
    )
```

```python
import functools
import math

import jax
import jax.numpy as jnp
from jax import lax
from jax.experimental import pallas as pl
from jax.experimental.pallas import tpu as pltpu
from jax.sharding import PartitionSpec as P

f32, bf16 = jnp.float32, jnp.bfloat16
LANES, SUB = 128, 8

WAVE_NUMBER = 8.0
NEAR = 3
SINE = [(-1.0) ** k * (2.0 * math.pi) ** (2 * k + 1) / math.factorial(2 * k + 1) for k in range(7)]
NN = (((1,), (0,)), ((), ()))
NT = (((1,), (1,)), ((), ()))
TN = (((0,), (0,)), ((), ()))


def dot(a, b, dims):
    return lax.dot_general(a, b, dims, preferred_element_type=f32)


def split(x):
    hi = x.astype(bf16)
    return hi, (x - hi.astype(f32)).astype(bf16)


def dot3(a, b, dims):
    ah, al = a if isinstance(a, tuple) else split(a)
    bh, bl = b if isinstance(b, tuple) else split(b)
    return dot(ah, bh, dims) + (dot(al, bh, dims) + dot(ah, bl, dims))


def row_bcast(x, j):
    return jnp.broadcast_to(x[j : j + 1, :], x.shape)


def lane_bcast(x, k):
    return jnp.broadcast_to(x[:, k : k + 1], x.shape)


def eliminate(many, groups, zero, near, between=None):
    shape = many[0][0].shape
    sub = lax.broadcasted_iota(jnp.int32, shape, 0)
    lane = lax.broadcasted_iota(jnp.int32, shape, 1)
    diagonals = [[lane_bcast(mats[0], t) + zero for t in range(SUB)] for mats in many]
    for g in range(groups):
        for which, mats in enumerate(many):
            diag = diagonals[which]
            more = g + 1 < groups
            if more:
                under = [lane_bcast(mats[g + 1], SUB * g + t) for t in range(SUB)]
                under[0] = under[0] + zero
                ahead = [lane_bcast(mats[g + 1], SUB * (g + 1) + t) for t in range(SUB)]
            rows, heads, scale = [], [], None
            for j in range(SUB):
                c = diag[j]
                root = lax.rsqrt(row_bcast(c, j))
                inv = root * root
                below = jnp.where(sub > j, c, 0.0)
                head = {}
                for t in range(j + 1, SUB):
                    raw = row_bcast(c, t)
                    head[t] = raw * inv
                    diag[t] = diag[t] - ((below * raw) * inv if t == j + 1 else below * head[t])
                row = row_bcast(mats[g], j) * jnp.where(lane == SUB * g + j, inv + inv, inv)
                mats[g] = mats[g] - below * row
                scale = root if j == 0 else jnp.where(sub == j, root, scale)
                rows.append(row)
                heads.append(head)
                if more:
                    c = under[j]
                    scaled = c * inv
                    for t in range(j + 1, SUB):
                        under[t] = under[t] - c * head[t]
                    for t in range(SUB):
                        ahead[t] = ahead[t] - scaled * row_bcast(c, t)
                    mats[g + 1] = mats[g + 1] - c * row
            mats[g] = mats[g] * scale
            if g + near + 1 < groups:
                inside = (lane >= SUB * g) & (lane < SUB * (g + 1))
                high, low = split(mats[g])
                right = jnp.where(inside & (lane > SUB * g + sub), 0.0, mats[g])
                right_high, right_low = split(right)
                none = jnp.zeros_like(high)
                product = dot(
                    jnp.concatenate([high, high, low, none], 0),
                    jnp.concatenate([right_high, right_low, right_high, none], 0),
                    TN,
                )
                for i in range(g + near + 1, groups):
                    mats[i] = jnp.where(inside, 0.0, mats[i]) - product[SUB * i : SUB * (i + 1), :]
            for i in range(g + 2, min(groups, g + near + 1)):
                p = [lane_bcast(mats[i], SUB * g + t) for t in range(SUB)]
                for j in range(SUB):
                    for t in range(j + 1, SUB):
                        p[t] = p[t] - p[j] * heads[j][t]
                    mats[i] = mats[i] - p[j] * rows[j]
            if more:
                diagonals[which] = ahead
        if between:
            between(g)


def factors_of(mats, size):
    both = jnp.concatenate(mats, 0)[:, :size]
    r = lax.broadcasted_iota(jnp.int32, (size, size), 0)
    c = lax.broadcasted_iota(jnp.int32, (size, size), 1)
    root = jnp.sum(jnp.where(r == c, both, 0.0), axis=0, keepdims=True)
    inv = lax.rsqrt(root * root)
    return both, jnp.where(c <= r, both * (inv * inv), 0.0)


def pair(x):
    return jnp.concatenate(split(x), 1)


def times(a, b):
    high, low = b
    k, n = high.shape
    right = jnp.concatenate(
        [jnp.concatenate([high, low], 1), jnp.concatenate([high, jnp.zeros_like(low)], 1)], 0
    )
    out = dot(a, right, NN)
    return out[:, :n] + out[:, n:]


def times_t(a, b):
    high, low = b
    n, k = high.shape
    right = jnp.concatenate(
        [jnp.concatenate([high, high], 1), jnp.concatenate([low, jnp.zeros_like(low)], 1)], 0
    )
    out = dot(a, right, NT)
    return out[:, :n] + out[:, n:]


def chol_kernel(ucat_ref, basis_ref, tri_ref, a_ref, o_ref, y_ref, d_ref, l_ref, x_ref, p_ref, sems):
    n, inner = ucat_ref.shape
    blk = LANES
    nb = n // blk
    wide = 2 * blk
    groups = blk // SUB
    col = lax.axis_index("col")
    own = pl.ds(pl.multiple_of(col * blk, blk), blk)
    row_id = lax.broadcasted_iota(jnp.int32, (blk, blk), 0)
    col_id = lax.broadcasted_iota(jnp.int32, (blk, blk), 1)
    eye = row_id == col_id
    tiles = [(slice(r, r + wide), slice(c, c + wide)) for c in range(0, n, wide) for r in range(c, n, wide)]

    squares = jnp.zeros((SUB, inner), f32)
    for i in range(0, n, blk):
        top = ucat_ref[i : i + blk, :].astype(f32)
        squares = squares + jnp.sum((top * top).reshape(blk // SUB, SUB, inner), axis=0)
    shift = jnp.sum(squares) * (1.0 / (inner * n)) + 1e-06
    zero = jnp.zeros((SUB, LANES), f32) + shift * 0.0

    def diagonal(d, steps):
        d = d + jnp.where(eye, shift, 0.0)
        mats = [d[SUB * i : SUB * (i + 1), :] for i in range(groups)]
        steps = list(steps)
        turns = [steps[len(steps) * g // groups : len(steps) * (g + 1) // groups] for g in range(groups)]

        def between(g):
            for step in turns[g]:
                step()

        eliminate([mats], groups, zero, NEAR, between)
        both, inverse = factors_of(mats, blk)
        return jnp.where(row_id <= col_id, both, 0.0).T, split(inverse)

    def spread(low, xs, b):
        nxt = jnp.minimum(b + 1, nb - 1)
        under = pl.ds(pl.multiple_of(nxt * blk, blk), blk)
        here = pl.ds(pl.multiple_of(b * blk, blk), blk)
        below = split(times_t(pair(a_ref[under, here]), xs))
        d_ref[...] = a_ref[under, under] - times_t(jnp.concatenate(below, 1), below)
        l_ref[...] = low
        x_ref[0] = xs[0]
        x_ref[1] = xs[1]

    def copy_out(b):
        strip = pl.ds(pl.multiple_of(b * blk, blk), blk)
        return pltpu.make_async_copy(o_ref.at[b], tri_ref.at[0, :, strip], sems.at[b])

    y_ref[...] = ucat_ref[:, own].astype(f32)

    def gram(rows, cols):
        return dot(ucat_ref[rows, :], ucat_ref[cols, :], NT) * (1.0 / inner)

    def gram_step(rows, cols):
        a_ref[rows, cols] = gram(rows, cols)

    corner = slice(0, blk)
    low, xs = diagonal(gram(corner, corner), [functools.partial(gram_step, *t) for t in tiles])
    spread(low, xs, 0)

    def block(b, carry):
        done = b - 1
        at = pl.ds(pl.multiple_of(done * blk, blk), blk)
        xs_old = (x_ref[0], x_ref[1])
        first = b * blk
        later = {}

        def solve_rows():
            yb = times(jnp.concatenate(xs_old, 1), split(y_ref[at, :]))
            basis_ref[0, at, :] = yb.astype(bf16)
            later["y"] = split(yb)

        def panel(r):
            rows = slice(r, r + wide)
            p = times_t(pair(a_ref[rows, at]), xs_old)
            ids = lax.broadcasted_iota(jnp.int32, (wide, blk), 0) + r
            p = jnp.where(ids >= first, p, 0.0)
            o_ref[done, rows, :] = p
            p_ref[rows, :] = pair(p)

        def trail(rows, cols):
            left = p_ref[rows, :]
            high, low = p_ref[cols, :blk], p_ref[cols, blk:]
            left = jnp.concatenate([left, left[:, :blk]], 1)
            a_ref[rows, cols] -= dot(left, jnp.concatenate([high, high, low], 1), NT)

        def rest(r):
            rows = slice(r, r + wide)
            y_ref[rows, :] -= times(p_ref[rows, :], later["y"])

        steps = [solve_rows]
        steps += [functools.partial(panel, r) for r in range(0, n, wide)]
        steps += [functools.partial(trail, *t) for t in tiles]
        steps += [functools.partial(rest, r) for r in range(0, n, wide)]
        low, xs = diagonal(d_ref[...], steps)
        o_ref[done, at, :] = l_ref[...]
        copy_out(done).start()
        spread(low, xs, b)
        return carry

    lax.fori_loop(1, nb, block, 0)
    last = slice(n - blk, n)
    o_ref[nb - 1, 0 : n - blk, :] = jnp.zeros((n - blk, blk), f32)
    o_ref[nb - 1, last, :] = l_ref[...]
    copy_out(nb - 1).start()
    xs = jnp.concatenate([x_ref[0], x_ref[1]], 1)
    basis_ref[0, last, :] = times(xs, split(y_ref[last, :])).astype(bf16)
    for b in range(nb):
        copy_out(b).wait()


def factor(ucat, part):
    n, inner = ucat.shape
    vmem = pl.BlockSpec(memory_space=pltpu.VMEM)
    return pl.pallas_call(
        chol_kernel,
        out_shape=(
            jax.ShapeDtypeStruct((1, n, part), bf16),
            jax.ShapeDtypeStruct((1, n, n), f32),
        ),
        in_specs=[vmem],
        out_specs=(vmem, pl.BlockSpec(memory_space=pl.ANY)),
        scratch_shapes=[
            pltpu.VMEM((n, n), f32),
            pltpu.VMEM((n // LANES, n, LANES), f32),
            pltpu.VMEM((n, part), f32),
            pltpu.VMEM((LANES, LANES), f32),
            pltpu.VMEM((LANES, LANES), f32),
            pltpu.VMEM((2, LANES, LANES), bf16),
            pltpu.VMEM((n, 2 * LANES), bf16),
            pltpu.SemaphoreType.DMA((n // LANES,)),
        ],
        compiler_params=pltpu.CompilerParams(vmem_limit_bytes=48 << 20),
        name="factor",
    )(ucat)


def wave(a, b):
    dx, dy, dz = a[0] - b[0], a[1] - b[1], a[2] - b[2]
    square = dx * dx + dy * dy + dz * dz
    inverse = lax.rsqrt(square)
    turns = square * inverse * (WAVE_NUMBER / (2.0 * math.pi))
    rest = jnp.abs(turns - jnp.floor(turns + 0.5))
    x = 0.25 - rest
    xx = x * x
    poly = SINE[-1]
    for c in SINE[-2::-1]:
        poly = poly * xx + c
    return a[3] * b[3] * (poly * x * inverse)


def shifted_inverse(tops):
    rank = tops[0].shape[0]
    groups = rank // SUB
    r = lax.broadcasted_iota(jnp.int32, (rank, rank), 0)
    c = lax.broadcasted_iota(jnp.int32, (rank, rank), 1)
    all_rows = []
    for top in tops:
        s = split(top)
        shift = jnp.sum(top * top) * (1.0 / rank) + 1e-06
        normal = dot3(s, s, NT) + jnp.where(r == c, shift, 0.0)
        normal = jnp.concatenate([normal, jnp.zeros((rank, LANES - rank), f32)], 1)
        all_rows.append([normal[SUB * i : SUB * (i + 1), :] for i in range(groups)])
    eliminate(all_rows, groups, jnp.zeros((SUB, LANES), f32) + jnp.max(tops[0]) * 0.0, groups)
    return [factors_of(rows, rank)[1] for rows in all_rows]


def cross_kernel(rank, far_ref, tile_ref, ucat_ref, right_ref, pts_ref, ij_ref, ijt_ref, c_ref, v_ref):
    devices = tile_ref.shape[0]
    cols = lax.axis_size("col")
    clusters = devices // cols
    size = cols * LANES
    local = far_ref.shape[1]
    slots = cols * local
    row, col = lax.axis_index("row"), lax.axis_index("col")

    for k in range(clusters):
        p = jnp.concatenate([tile_ref[k * cols + c, 0:4, :] for c in range(cols)], 1)
        hi, mid = split(p)
        lo = (p - hi.astype(f32) - mid.astype(f32)).astype(bf16)
        zero = jnp.zeros((4, size), bf16)
        pts_ref[16 * k : 16 * k + 16, :] = jnp.concatenate([hi, mid, lo, zero], 0)

    spots = lax.broadcasted_iota(jnp.int32, (size, LANES), 0)
    of = lax.broadcasted_iota(jnp.int32, (clusters, 16, LANES), 0)
    for c in range(cols):
        for s in range(local):
            found = []
            for kind in range(2):
                panel = tile_ref[row * cols + c, 4 + kind * local + s : 5 + kind * local + s, :].astype(jnp.int32)
                where = panel // size
                hot = jnp.where(spots == panel - where * size, 1.0, 0.0).astype(bf16)
                got = dot(pts_ref[...], hot, NN).reshape(clusters, 16, LANES)
                got = jnp.sum(jnp.where(of == where[None], got, 0.0), axis=0)
                found.append(got[0:4] + got[4:8] + got[8:12])
            at = 8 * (c * local + s)
            ij_ref[at : at + 8, :] = jnp.concatenate(found, 0)
    ijt_ref[...] = jnp.concatenate([ij_ref[...], jnp.zeros((LANES - 8 * slots, LANES), f32)], 0).T

    own = jnp.concatenate([tile_ref[row * cols + c, 0:4, :] for c in range(cols)], 1)
    own = [own[i : i + 1, :] for i in range(4)]

    def as_rows(slot, kind, k):
        at = 8 * slot + 4 * kind
        return [ij_ref[at + i : at + i + 1, k * rank : (k + 1) * rank] for i in range(4)]

    def as_columns(slot, kind, k):
        at = 8 * slot + 4 * kind
        return [ijt_ref[k * rank : (k + 1) * rank, at + i : at + i + 1] for i in range(4)]

    group = 4
    for first in range(0, slots, group):
        tops = [wave(as_columns(s, 1, 0), as_rows(s, 0, 0)) for s in range(first, first + group)]
        lowers = shifted_inverse(tops)
        for s, top, lower in zip(range(first, first + group), tops, lowers):
            low = split(lower)
            half = dot3(low, split(top), NN)
            coupling = dot3(low, split(half), TN)
            c_ref[s] = coupling
            v_t = dot3(split(wave(as_columns(s, 1, 1), as_rows(s, 0, 0))), split(coupling), NT).astype(bf16)
            v_ref[s] = v_t
            at = s * 2 * rank
            u0 = wave(as_columns(s, 1, 0), own).astype(bf16)
            ucat_ref[at : at + rank, :] = u0
            u1 = wave(as_columns(s, 1, 1), own) - dot(v_t, u0, NN)
            ucat_ref[at + rank : at + 2 * rank, :] = u1.astype(bf16)

    tops, rest = [], []
    for s in range(local):
        slot = col * local + s
        rows = ij_ref[pl.ds(pl.multiple_of(8 * slot, 8), 8), :]
        columns = rows.T
        i_row = [[rows[q : q + 1, k * rank : (k + 1) * rank] for q in range(4)] for k in range(2)]
        j_row = [[rows[4 + q : 5 + q, k * rank : (k + 1) * rank] for q in range(4)] for k in range(2)]
        i_col = [[columns[k * rank : (k + 1) * rank, q : q + 1] for q in range(4)] for k in range(2)]
        j_col = [[columns[k * rank : (k + 1) * rank, 4 + q : 5 + q] for q in range(4)] for k in range(2)]
        far = far_ref[0, s]
        there = jnp.concatenate([tile_ref[far * cols + c, 0:4, :] for c in range(cols)], 1)
        there = [there[q : q + 1, :] for q in range(4)]
        v0 = dot3(split(c_ref[slot]), split(wave(i_col[0], there)), NN).astype(bf16)
        at = s * 2 * rank
        right_ref[0, at : at + rank, :] = v0
        u_t = wave(i_col[1], j_row[0]).astype(bf16)
        row_panel = wave(i_col[1], there) - dot(u_t, v0, NN)
        u_i = wave(j_col[0], i_row[1]).astype(bf16)
        tops.append(wave(j_col[1], i_row[1]) - dot(v_ref[slot], u_i, NN))
        rest.append(row_panel)
    lowers = shifted_inverse(tops)
    for s in range(local):
        low = split(lowers[s])
        coupling = dot3(low, split(dot3(low, split(tops[s]), NN)), TN)
        at = (2 * s + 1) * rank
        right_ref[0, at : at + rank, :] = dot3(split(coupling), split(rest[s]), NN).astype(bf16)


def cross(far_blocks, tiles, rank, cols):
    local = far_blocks.shape[1]
    slots = cols * local
    clusters = tiles.shape[0] // cols
    size = cols * LANES
    vmem = pl.BlockSpec(memory_space=pltpu.VMEM)
    return pl.pallas_call(
        functools.partial(cross_kernel, rank),
        out_shape=(
            jax.ShapeDtypeStruct((slots * 2 * rank, size), bf16),
            jax.ShapeDtypeStruct((1, local * 2 * rank, size), bf16),
        ),
        in_specs=[pl.BlockSpec(memory_space=pltpu.SMEM), vmem],
        out_specs=(vmem, vmem),
        scratch_shapes=[
            pltpu.VMEM((16 * clusters, size), bf16),
            pltpu.VMEM((8 * slots, LANES), f32),
            pltpu.VMEM((LANES, LANES), f32),
            pltpu.VMEM((slots, rank, rank), f32),
            pltpu.VMEM((slots, rank, rank), bf16),
        ],
        compiler_params=pltpu.CompilerParams(vmem_limit_bytes=48 << 20),
        name="cross",
    )(far_blocks, tiles)


def per_device(points, weights, far_blocks, row_pivots, col_pivots):
    part = points.shape[1]
    cols = lax.axis_size("col")
    size = part * cols
    rank = row_pivots.shape[3]
    own = row_pivots[0] + lax.axis_index("row") * size
    far = col_pivots[0] + far_blocks[0][:, None, None] * size
    tile = jnp.concatenate(
        [points, weights[None], own.reshape(-1, part).astype(f32), far.reshape(-1, part).astype(f32)], 0
    )
    count = lax.axis_size("row") * cols
    tiles = lax.all_to_all(
        jnp.broadcast_to(tile[None], (count,) + tile.shape), ("row", "col"), split_axis=0, concat_axis=0, tiled=True
    )
    ucat, factors_v = cross(far_blocks, tiles, rank, cols)
    basis, lower = factor(ucat, part)
    return factors_v, basis, lower


def solution(mesh):
    return jax.shard_map(
        per_device,
        mesh=mesh,
        in_specs=(
            P(None, ("row", "col")),
            P(("row", "col")),
            P("row", "col"),
            P("row", "col", None, None),
            P("row", "col", None, None),
        ),
        out_specs=(P("row", "col", None), P("row", None, "col"), P("row", None, None)),
        check_vma=False,
    )
```

```python
import functools
import math

import jax
import jax.numpy as jnp
from jax import lax
from jax.experimental import pallas as pl
from jax.experimental.pallas import tpu as pltpu
from jax.sharding import PartitionSpec as P

f32, bf16 = jnp.float32, jnp.bfloat16
LANES, SUB = 128, 8

WAVE_NUMBER = 8.0
NEAR = 3
SINE = [6.283185273658022, -41.341677416633885, 81.60222657697675, -76.5748772418381, 39.71002372452099]
NN = (((1,), (0,)), ((), ()))
NT = (((1,), (1,)), ((), ()))
TN = (((0,), (0,)), ((), ()))


def dot(a, b, dims):
    return lax.dot_general(a, b, dims, preferred_element_type=f32)


def split(x):
    hi = x.astype(bf16)
    return hi, (x - hi.astype(f32)).astype(bf16)


def dot3(a, b, dims):
    ah, al = a if isinstance(a, tuple) else split(a)
    bh, bl = b if isinstance(b, tuple) else split(b)
    return dot(ah, bh, dims) + (dot(al, bh, dims) + dot(ah, bl, dims))


def row_bcast(x, j):
    return jnp.broadcast_to(x[j : j + 1, :], x.shape)


def eliminate(many, groups, near, width=LANES, zero=None, between=None):
    shape = many[0][0].shape
    sub = lax.broadcasted_iota(jnp.int32, shape, 0)
    lane = lax.broadcasted_iota(jnp.int32, shape, 1)
    start, spot = lane // width * width, lane % width
    look = zero is not None

    def lane_bcast(x, k):
        if width == LANES:
            return jnp.broadcast_to(x[:, k : k + 1], x.shape)
        return jnp.take_along_axis(x, start + k, axis=1, mode="promise_in_bounds")

    diagonals = [[lane_bcast(mats[0], t) + zero for t in range(SUB)] if look else None for mats in many]
    for g in range(groups):
        last = min(groups, g + near + 1)
        more = look and g + 1 < groups
        panels = [{} for _ in many]
        aheads = [{} for _ in many]
        for t in range(SUB):
            for mats, panel in zip(many, panels):
                for i in range(g + 1 if look else g, last):
                    panel[i, t] = lane_bcast(mats[i], SUB * g + t)
            for mats, ahead in zip(many, aheads):
                if more:
                    ahead[t] = lane_bcast(mats[g + 1], SUB * (g + 1) + t)
        for which, (mats, panel, ahead) in enumerate(zip(many, panels, aheads)):
            if look:
                diag = diagonals[which]
            else:
                diag = [panel[g, t] for t in range(SUB)]
            if more:
                panel[g + 1, 0] = panel[g + 1, 0] + zero
            rows, heads, scale = [], [], None
            for j in range(SUB):
                c = diag[j]
                root = lax.rsqrt(row_bcast(c, j))
                inv = root * root
                below = jnp.where(sub > j, c, 0.0)
                head = {}
                for t in range(j + 1, SUB):
                    raw = row_bcast(c, t)
                    head[t] = raw * inv
                    diag[t] = diag[t] - ((below * raw) * inv if t == j + 1 else below * head[t])
                row = row_bcast(mats[g], j) * jnp.where(spot == SUB * g + j, inv + inv, inv)
                mats[g] = mats[g] - below * row
                scale = root if j == 0 else jnp.where(sub == j, root, scale)
                rows.append(row)
                heads.append(head)
                if more:
                    c = panel[g + 1, j]
                    scaled = c * inv
                    for t in range(j + 1, SUB):
                        panel[g + 1, t] = panel[g + 1, t] - c * head[t]
                    for t in range(SUB):
                        ahead[t] = ahead[t] - scaled * row_bcast(c, t)
                    mats[g + 1] = mats[g + 1] - c * row
            mats[g] = mats[g] * scale
            if last < groups:
                inside = (lane >= SUB * g) & (lane < SUB * (g + 1))
                high, low = split(mats[g])
                right = jnp.where(inside & (lane > SUB * g + sub), 0.0, mats[g])
                right_high, right_low = split(right)
                none = jnp.zeros_like(high)
                product = dot(
                    jnp.concatenate([high, high, low, none], 0),
                    jnp.concatenate([right_high, right_low, right_high, none], 0),
                    TN,
                )
                for i in range(last, groups):
                    mats[i] = jnp.where(inside, 0.0, mats[i]) - product[SUB * i : SUB * (i + 1), :]
            for i in range(g + 2 if look else g + 1, last):
                for j in range(SUB):
                    for t in range(j + 1, SUB):
                        panel[i, t] = panel[i, t] - panel[i, j] * heads[j][t]
                    mats[i] = mats[i] - panel[i, j] * rows[j]
            diagonals[which] = ahead
        if between:
            between(g)


def factors_of(mats, width=LANES):
    both = jnp.concatenate(mats, 0)
    r = lax.broadcasted_iota(jnp.int32, both.shape, 0)
    c = lax.broadcasted_iota(jnp.int32, both.shape, 1) % width
    root = jnp.sum(jnp.where(r == c, both, 0.0), axis=0, keepdims=True)
    inv = lax.rsqrt(root * root)
    return both, jnp.where(c <= r, both * (inv * inv), 0.0)


def in_turns(steps, count):
    return [steps[len(steps) * g // count : len(steps) * (g + 1) // count] for g in range(count)]


def pair(x):
    return jnp.concatenate(split(x), 1)


def times(a, b):
    high, low = b
    k, n = high.shape
    right = jnp.concatenate(
        [jnp.concatenate([high, low], 1), jnp.concatenate([high, jnp.zeros_like(low)], 1)], 0
    )
    out = dot(a, right, NN)
    return out[:, :n] + out[:, n:]


def times_t(a, b):
    high, low = b
    n, k = high.shape
    right = jnp.concatenate(
        [jnp.concatenate([high, high], 1), jnp.concatenate([low, jnp.zeros_like(low)], 1)], 0
    )
    out = dot(a, right, NT)
    return out[:, :n] + out[:, n:]


def chol_kernel(ucat_ref, basis_ref, tri_ref, a_ref, o_ref, y_ref, d_ref, l_ref, x_ref, p_ref, sems):
    n, inner = ucat_ref.shape
    blk = LANES
    nb = n // blk
    wide = 2 * blk
    groups = blk // SUB
    col = lax.axis_index("col")
    own = pl.ds(pl.multiple_of(col * blk, blk), blk)
    row_id = lax.broadcasted_iota(jnp.int32, (blk, blk), 0)
    col_id = lax.broadcasted_iota(jnp.int32, (blk, blk), 1)
    eye = row_id == col_id
    tiles = [(slice(r, r + wide), slice(c, c + wide)) for c in range(0, n, wide) for r in range(c, n, wide)]

    squares = jnp.zeros((SUB, inner), f32)
    for i in range(0, n, blk):
        top = ucat_ref[i : i + blk, :].astype(f32)
        squares = squares + jnp.sum((top * top).reshape(blk // SUB, SUB, inner), axis=0)
    shift = jnp.sum(squares) * (1.0 / (inner * n)) + 1e-06
    zero = jnp.zeros((SUB, LANES), f32) + shift * 0.0

    def diagonal(d, steps):
        d = d + jnp.where(eye, shift, 0.0)
        mats = [d[SUB * i : SUB * (i + 1), :] for i in range(groups)]
        turns = steps

        def between(g):
            for step in turns[g]:
                step()

        eliminate([mats], groups, NEAR, LANES, zero, between)
        both, inverse = factors_of(mats)
        return jnp.where(row_id <= col_id, both, 0.0).T, split(inverse)

    def spread(low, xs, b):
        nxt = jnp.minimum(b + 1, nb - 1)
        under = pl.ds(pl.multiple_of(nxt * blk, blk), blk)
        here = pl.ds(pl.multiple_of(b * blk, blk), blk)
        below = split(times_t(pair(a_ref[under, here]), xs))
        d_ref[...] = a_ref[under, under] - times_t(jnp.concatenate(below, 1), below)
        l_ref[...] = low
        x_ref[0] = xs[0]
        x_ref[1] = xs[1]

    def copy_out(b):
        strip = pl.ds(pl.multiple_of(b * blk, blk), blk)
        return pltpu.make_async_copy(o_ref.at[b], tri_ref.at[0, :, strip], sems.at[b])

    y_ref[...] = ucat_ref[:, own].astype(f32)

    def gram(rows, cols):
        return dot(ucat_ref[rows, :], ucat_ref[cols, :], NT) * (1.0 / inner)

    def gram_step(rows, cols):
        a_ref[rows, cols] = gram(rows, cols)

    corner = slice(0, blk)
    low, xs = diagonal(gram(corner, corner), in_turns([functools.partial(gram_step, *t) for t in tiles], groups))
    spread(low, xs, 0)

    def block(b, carry):
        done = b - 1
        at = pl.ds(pl.multiple_of(done * blk, blk), blk)
        xs_old = (x_ref[0], x_ref[1])
        first = b * blk
        later = {}

        def solve_rows():
            yb = times(jnp.concatenate(xs_old, 1), split(y_ref[at, :]))
            basis_ref[0, at, :] = yb.astype(bf16)
            later["y"] = split(yb)

        def panel(r):
            rows = slice(r, r + wide)
            p = times_t(pair(a_ref[rows, at]), xs_old)
            ids = lax.broadcasted_iota(jnp.int32, (wide, blk), 0) + r
            p = jnp.where(ids >= first, p, 0.0)
            o_ref[done, rows, :] = p
            p_ref[rows, :] = pair(p)

        def trail(rows, cols):
            left = p_ref[rows, :]
            high, low = p_ref[cols, :blk], p_ref[cols, blk:]
            left = jnp.concatenate([left, left[:, :blk]], 1)
            a_ref[rows, cols] -= dot(left, jnp.concatenate([high, high, low], 1), NT)

        def rest(r):
            rows = slice(r, r + wide)
            y_ref[rows, :] -= times(p_ref[rows, :], later["y"])

        panels = [functools.partial(panel, r) for r in range(0, n, wide)]
        trails = [functools.partial(trail, *t) for t in tiles]
        rests = [functools.partial(rest, r) for r in range(0, n, wide)]
        steps = in_turns(panels, 2) + [[solve_rows]] + in_turns(trails + rests, groups - 3)
        low, xs = diagonal(d_ref[...], steps)
        o_ref[done, at, :] = l_ref[...]
        copy_out(done).start()
        spread(low, xs, b)
        return carry

    lax.fori_loop(1, nb, block, 0)
    last = slice(n - blk, n)
    o_ref[nb - 1, 0 : n - blk, :] = jnp.zeros((n - blk, blk), f32)
    o_ref[nb - 1, last, :] = l_ref[...]
    copy_out(nb - 1).start()
    xs = jnp.concatenate([x_ref[0], x_ref[1]], 1)
    basis_ref[0, last, :] = times(xs, split(y_ref[last, :])).astype(bf16)
    for b in range(nb):
        copy_out(b).wait()


def factor(ucat, part):
    n, inner = ucat.shape
    vmem = pl.BlockSpec(memory_space=pltpu.VMEM)
    return pl.pallas_call(
        chol_kernel,
        out_shape=(
            jax.ShapeDtypeStruct((1, n, part), bf16),
            jax.ShapeDtypeStruct((1, n, n), f32),
        ),
        in_specs=[vmem],
        out_specs=(vmem, pl.BlockSpec(memory_space=pl.ANY)),
        scratch_shapes=[
            pltpu.VMEM((n, n), f32),
            pltpu.VMEM((n // LANES, n, LANES), f32),
            pltpu.VMEM((n, part), f32),
            pltpu.VMEM((LANES, LANES), f32),
            pltpu.VMEM((LANES, LANES), f32),
            pltpu.VMEM((2, LANES, LANES), bf16),
            pltpu.VMEM((n, 2 * LANES), bf16),
            pltpu.SemaphoreType.DMA((n // LANES,)),
        ],
        compiler_params=pltpu.CompilerParams(vmem_limit_bytes=48 << 20),
        name="factor",
    )(ucat)


def wave(a, b):
    dx, dy, dz = a[0] - b[0], a[1] - b[1], a[2] - b[2]
    square = dx * dx + dy * dy + dz * dz
    inverse = lax.rsqrt(square)
    turns = square * inverse * (WAVE_NUMBER / (2.0 * math.pi))
    x = 0.25 - jnp.abs(turns - lax.round(turns, lax.RoundingMethod.TO_NEAREST_EVEN))
    xx = x * x
    poly = SINE[-1]
    for c in SINE[-2::-1]:
        poly = poly * xx + c
    return (a[3] * b[3]) * (poly * x * inverse)


def apart(x, left):
    none = jnp.zeros_like(x)
    return jnp.concatenate([jnp.where(left, x, none), jnp.where(left, none, x)], 0)


def shifted_inverse(tops, look, fillers):
    rank = tops[0].shape[0]
    groups = rank // SUB
    r = lax.broadcasted_iota(jnp.int32, tops[0].shape, 0)
    c = lax.broadcasted_iota(jnp.int32, tops[0].shape, 1)
    left = c < rank
    mats = []
    for top in tops:
        normal = times_t(pair(top), split(apart(top, left)))
        squares = jnp.sum(top * top, axis=0, keepdims=True)
        first = lax.broadcasted_iota(jnp.int32, squares.shape, 1) < rank
        shift = [jnp.sum(jnp.where(first == side, squares, 0.0), axis=1, keepdims=True) for side in (True, False)]
        shift = jnp.where(first, shift[0], shift[1]) * (1.0 / rank) + 1e-06
        normal = normal + jnp.where(r == c % rank, shift, 0.0)
        mats.append([normal[SUB * i : SUB * (i + 1), :] for i in range(groups)])
    zero = jnp.zeros((SUB, LANES), f32) + jnp.max(tops[0]) * 0.0 if look else None
    turns = in_turns(fillers, groups)

    def between(g):
        for step in turns[g]:
            step()

    eliminate(mats, groups, groups, rank, zero, between)
    return [factors_of(rows, rank)[1] for rows in mats]


def cross_kernel(rank, far_ref, tile_ref, ucat_ref, right_ref, pts_ref, ij_ref, ijt_ref, low_ref, half_ref, v_ref, panel_ref):
    devices = tile_ref.shape[0]
    cols = lax.axis_size("col")
    clusters = devices // cols
    size = cols * LANES
    local = far_ref.shape[1]
    slots = cols * local
    row, col = lax.axis_index("row"), lax.axis_index("col")
    left = lax.broadcasted_iota(jnp.int32, (rank, LANES), 1) < rank

    for k in range(clusters):
        p = jnp.concatenate([tile_ref[k * cols + c, 0:4, :] for c in range(cols)], 1)
        hi, mid = split(p)
        lo = (p - hi.astype(f32) - mid.astype(f32)).astype(bf16)
        zero = jnp.zeros((4, size), bf16)
        pts_ref[16 * k : 16 * k + 16, :] = jnp.concatenate([hi, mid, lo, zero], 0)

    spots = lax.broadcasted_iota(jnp.int32, (size, LANES), 0)
    of = lax.broadcasted_iota(jnp.int32, (clusters, 16, LANES), 0)
    for c in range(cols):
        for s in range(local):
            found = []
            for kind in range(2):
                panel = tile_ref[row * cols + c, 4 + kind * local + s : 5 + kind * local + s, :].astype(jnp.int32)
                where = panel // size
                hot = jnp.where(spots == panel - where * size, 1.0, 0.0).astype(bf16)
                got = dot(pts_ref[...], hot, NN).reshape(clusters, 16, LANES)
                got = jnp.sum(jnp.where(of == where[None], got, 0.0), axis=0)
                found.append(got[0:4] + got[4:8] + got[8:12])
            at = 8 * (c * local + s)
            ij_ref[at : at + 8, :] = jnp.concatenate(found, 0)
    ijt_ref[...] = jnp.concatenate([ij_ref[...], jnp.zeros((LANES - 8 * slots, LANES), f32)], 0).T

    def points_of(tile):
        both = jnp.concatenate([tile_ref[tile * cols + c, 0:4, :] for c in range(cols)], 1)
        return [both[i : i + 1, :] for i in range(4)]

    def columns(source, at, k):
        part = source[k * rank : (k + 1) * rank, :]
        return [jnp.broadcast_to(part[:, at + i : at + i + 1], (rank, LANES)) for i in range(4)]

    def both_rows(a, b, k):
        first = lax.broadcasted_iota(jnp.int32, (4, LANES), 1) < rank
        a, b = (b, a) if k else (a, b)
        other = pltpu.roll(b, rank, 1)
        got = jnp.where(first, other, a) if k else jnp.where(first, a, other)
        return [got[i : i + 1, :] for i in range(4)]

    def both_columns(a, b):
        return [jnp.where(left, x, y) for x, y in zip(a, b)]

    def against(column, points):
        wide = [jnp.concatenate([x] * cols, 1) for x in column]
        return wave(wide, points)

    own = points_of(row)

    pairs = []
    for s in range(0, slots, 2):
        rows_i = [ij_ref[8 * (s + h) : 8 * (s + h) + 4, :] for h in range(2)]
        j_cols = [[columns(ijt_ref, 8 * (s + h) + 4, k) for h in range(2)] for k in range(2)]
        i_rows = both_rows(rows_i[0], rows_i[1], 0)
        pairs.append([s, wave(both_columns(*j_cols[0]), i_rows), wave(both_columns(*j_cols[1]), i_rows), j_cols])

    mine = []
    for s in range(0, local, 2):
        which = (col * local + s) // 2
        rows = [ij_ref[pl.ds(pl.multiple_of(8 * (2 * which + h), 8), 8), :] for h in range(2)]
        flat = [r.T for r in rows]
        i_col = [[columns(flat[h], 0, k) for h in range(2)] for k in range(2)]
        j_col = [[columns(flat[h], 4, k) for h in range(2)] for k in range(2)]
        j_row = both_rows(rows[0][4:8], rows[1][4:8], 0)
        i_row = both_rows(rows[0][0:4], rows[1][0:4], 1)
        there = [points_of(far_ref[0, s + h]) for h in range(2)]
        mine.append((s, which, i_col, j_col, j_row, i_row, there))

    def left_factor(s, h, j_cols):
        at = (s + h) * 2 * rank
        ucat_ref[at : at + rank, :] = against(j_cols[0][h], own).astype(bf16)

    def row_panel(s, k, h, column, there):
        panel_ref[s // 2, k, h * rank : (h + 1) * rank, :] = against(column, there)

    def next_left_factor(s, j_cols):
        u0 = [ucat_ref[(s + h) * 2 * rank : (s + h) * 2 * rank + rank, :] for h in range(2)]
        product = dot(apart(v_ref[s // 2], left), jnp.concatenate(u0, 0), NN)
        for h in range(2):
            at = (s + h) * 2 * rank + rank
            u1 = against(j_cols[1][h], own) - product[h * rank : (h + 1) * rank]
            ucat_ref[at : at + rank, :] = u1.astype(bf16)

    fillers = [functools.partial(left_factor, p[0], h, p[3]) for p in pairs for h in range(2)]
    for s, _, i_col, _, _, _, there in mine:
        fillers += [
            functools.partial(row_panel, s, k, h, i_col[k][h], there[h]) for k in range(2) for h in range(2)
        ]
    lowers = shifted_inverse([p[1] for p in pairs], False, fillers)
    for (s, top, mixed, _), low in zip(pairs, lowers):
        half = times(pair(low), split(apart(top, left)))
        low_ref[s // 2] = low
        half_ref[s // 2] = half
        v_t = times_t(pair(mixed), split(apart(half, left)))
        v_ref[s // 2] = times(pair(v_t), split(apart(low, left))).astype(bf16)

    square = lax.broadcasted_iota(jnp.int32, (LANES, LANES), 0) < rank
    same = square == (lax.broadcasted_iota(jnp.int32, (LANES, LANES), 1) < rank)

    def couple(low, half, panel):
        coupling = jnp.where(same, dot3(split(low), split(half), TN), 0.0)
        high, low = split(coupling)
        panel_high, panel_low = split(panel)
        both = jnp.concatenate([high, low], 1)
        return dot(both, jnp.concatenate([panel_high, panel_high], 0), NN) + dot(high, panel_low, NN)

    fillers = [functools.partial(next_left_factor, p[0], p[3]) for p in pairs]
    for s, which, i_col, j_col, j_row, i_row, there in mine:
        top = wave(both_columns(*j_col[1]), i_row)
        u_i = wave(both_columns(*j_col[0]), i_row).astype(bf16)
        top = top - dot(v_ref[which], apart(u_i, left), NN)
        v0 = couple(low_ref[which], half_ref[which], panel_ref[s // 2, 0]).astype(bf16)
        u_t = wave(both_columns(*i_col[1]), j_row).astype(bf16)
        rest = panel_ref[s // 2, 1] - dot(apart(u_t, left), v0, NN)
        low = shifted_inverse([top], True, fillers[:len(pairs) - 1])[0]
        fillers = fillers[len(pairs) - 1:]
        v1 = couple(low, times(pair(low), split(apart(top, left))), rest).astype(bf16)
        for h in range(2):
            at = (s + h) * 2 * rank
            right_ref[0, at : at + rank, :] = v0[h * rank : (h + 1) * rank]
            right_ref[0, at + rank : at + 2 * rank, :] = v1[h * rank : (h + 1) * rank]
    for step in fillers:
        step()


def cross(far_blocks, tiles, rank, cols):
    local = far_blocks.shape[1]
    slots = cols * local
    clusters = tiles.shape[0] // cols
    size = cols * LANES
    vmem = pl.BlockSpec(memory_space=pltpu.VMEM)
    return pl.pallas_call(
        functools.partial(cross_kernel, rank),
        out_shape=(
            jax.ShapeDtypeStruct((slots * 2 * rank, size), bf16),
            jax.ShapeDtypeStruct((1, local * 2 * rank, size), bf16),
        ),
        in_specs=[pl.BlockSpec(memory_space=pltpu.SMEM), vmem],
        out_specs=(vmem, vmem),
        scratch_shapes=[
            pltpu.VMEM((16 * clusters, size), bf16),
            pltpu.VMEM((8 * slots, LANES), f32),
            pltpu.VMEM((LANES, LANES), f32),
            pltpu.VMEM((slots // 2, rank, LANES), f32),
            pltpu.VMEM((slots // 2, rank, LANES), f32),
            pltpu.VMEM((slots // 2, rank, LANES), bf16),
            pltpu.VMEM((local // 2, 2, 2 * rank, size), f32),
        ],
        compiler_params=pltpu.CompilerParams(vmem_limit_bytes=48 << 20),
        name="cross",
    )(far_blocks, tiles)


def pack_kernel(size, far_ref, points_ref, weights_ref, row_ref, col_ref, out_ref):
    local = far_ref.shape[1]
    first = lax.axis_index("row") * size
    own = [row_ref[0, s] + first for s in range(local)]
    far = [col_ref[0, s] + far_ref[0, s] * size for s in range(local)]
    flat = [jnp.concatenate([x[k : k + 1] for k in range(x.shape[0])], 1).astype(f32) for x in own + far]
    tile = jnp.concatenate([points_ref[...], weights_ref[...]] + flat, 0)
    out_ref[...] = jnp.broadcast_to(tile[None], out_ref.shape)


def pack(far_blocks, points, weights, row_pivots, col_pivots, count, size):
    vmem = pl.BlockSpec(memory_space=pltpu.VMEM)
    return pl.pallas_call(
        functools.partial(pack_kernel, size),
        out_shape=jax.ShapeDtypeStruct((count, 4 + 2 * far_blocks.shape[1], points.shape[1]), f32),
        in_specs=[pl.BlockSpec(memory_space=pltpu.SMEM), vmem, vmem, vmem, vmem],
        out_specs=vmem,
        name="pack",
    )(far_blocks, points, weights[None], row_pivots, col_pivots)


def per_device(points, weights, far_blocks, row_pivots, col_pivots):
    part = points.shape[1]
    cols = lax.axis_size("col")
    rank = row_pivots.shape[3]
    count = lax.axis_size("row") * cols
    tiles = pack(far_blocks, points, weights, row_pivots, col_pivots, count, part * cols)
    tiles = lax.all_to_all(tiles, ("row", "col"), split_axis=0, concat_axis=0, tiled=True)
    ucat, factors_v = cross(far_blocks, tiles, rank, cols)
    basis, lower = factor(ucat, part)
    return factors_v, basis, lower


def solution(mesh):
    return jax.shard_map(
        per_device,
        mesh=mesh,
        in_specs=(
            P(None, ("row", "col")),
            P(("row", "col")),
            P("row", "col"),
            P("row", "col", None, None),
            P("row", "col", None, None),
        ),
        out_specs=(P("row", "col", None), P("row", None, "col"), P("row", None, None)),
        check_vma=False,
    )
```

```python
import functools
import math

import jax
import jax.numpy as jnp
from jax import lax
from jax.experimental import pallas as pl
from jax.experimental.pallas import tpu as pltpu
from jax.sharding import PartitionSpec as P

f32, bf16 = jnp.float32, jnp.bfloat16
LANES, SUB = 128, 8

WAVE_NUMBER = 8.0
NEAR = 3
SINE = [6.283185273658022, -41.341677416633885, 81.60222657697675, -76.5748772418381, 39.71002372452099]
NN = (((1,), (0,)), ((), ()))
NT = (((1,), (1,)), ((), ()))
TN = (((0,), (0,)), ((), ()))


def dot(a, b, dims):
    return lax.dot_general(a, b, dims, preferred_element_type=f32)


def split(x):
    hi = x.astype(bf16)
    return hi, (x - hi.astype(f32)).astype(bf16)


def dot3(a, b, dims):
    ah, al = a if isinstance(a, tuple) else split(a)
    bh, bl = b if isinstance(b, tuple) else split(b)
    return dot(ah, bh, dims) + (dot(al, bh, dims) + dot(ah, bl, dims))


def row_bcast(x, j):
    return jnp.broadcast_to(x[j : j + 1, :], x.shape)


def eliminate(many, groups, near, width=LANES, zero=None):
    shape = many[0][0].shape
    sub = lax.broadcasted_iota(jnp.int32, shape, 0)
    lane = lax.broadcasted_iota(jnp.int32, shape, 1)
    start, spot = lane // width * width, lane % width
    look = zero is not None

    def lane_bcast(x, k):
        if width == LANES:
            return jnp.broadcast_to(x[:, k : k + 1], x.shape)
        return jnp.take_along_axis(x, start + k, axis=1, mode="promise_in_bounds")

    diagonals = [[lane_bcast(mats[0], t) + zero for t in range(SUB)] if look else None for mats in many]
    for g in range(groups):
        last = min(groups, g + near + 1)
        more = look and g + 1 < groups
        panels = [{} for _ in many]
        aheads = [{} for _ in many]
        for t in range(SUB):
            for mats, panel in zip(many, panels):
                for i in range(g + 1 if look else g, last):
                    panel[i, t] = lane_bcast(mats[i], SUB * g + t)
            for mats, ahead in zip(many, aheads):
                if more:
                    ahead[t] = lane_bcast(mats[g + 1], SUB * (g + 1) + t)
        for which, (mats, panel, ahead) in enumerate(zip(many, panels, aheads)):
            if look:
                diag = diagonals[which]
            else:
                diag = [panel[g, t] for t in range(SUB)]
            if more:
                panel[g + 1, 0] = panel[g + 1, 0] + zero
            rows, heads, scale = [], [], None
            for j in range(SUB):
                c = diag[j]
                root = lax.rsqrt(row_bcast(c, j))
                inv = root * root
                below = jnp.where(sub > j, c, 0.0)
                head = {}
                for t in range(j + 1, SUB):
                    raw = row_bcast(c, t)
                    head[t] = raw * inv
                    diag[t] = diag[t] - ((below * raw) * inv if t == j + 1 else below * head[t])
                row = row_bcast(mats[g], j) * jnp.where(spot == SUB * g + j, inv + inv, inv)
                mats[g] = mats[g] - below * row
                scale = root if j == 0 else jnp.where(sub == j, root, scale)
                rows.append(row)
                heads.append(head)
                if more:
                    c = panel[g + 1, j]
                    scaled = c * inv
                    for t in range(j + 1, SUB):
                        panel[g + 1, t] = panel[g + 1, t] - c * head[t]
                    for t in range(SUB):
                        ahead[t] = ahead[t] - scaled * row_bcast(c, t)
                    mats[g + 1] = mats[g + 1] - c * row
            mats[g] = mats[g] * scale
            if last < groups:
                inside = (spot >= SUB * g) & (spot < SUB * (g + 1))
                high, low = split(mats[g])
                right = jnp.where(inside & (spot > SUB * g + sub), 0.0, mats[g])
                right_high, right_low = split(right)
                none = jnp.zeros_like(high)
                product = dot(
                    jnp.concatenate([high, high, low, none], 0),
                    jnp.concatenate([right_high, right_low, right_high, none], 0),
                    TN,
                )
                for i in range(last, groups):
                    part = product[SUB * i : SUB * (i + 1), :]
                    for at in range(width, LANES, width):
                        part = jnp.where(lane < at, part, product[at + SUB * i : at + SUB * (i + 1), :])
                    mats[i] = jnp.where(inside, 0.0, mats[i]) - part
            for i in range(g + 2 if look else g + 1, last):
                for j in range(SUB):
                    for t in range(j + 1, SUB):
                        panel[i, t] = panel[i, t] - panel[i, j] * heads[j][t]
                    mats[i] = mats[i] - panel[i, j] * rows[j]
            diagonals[which] = ahead
        yield g


def factors_of(mats, width=LANES):
    both = jnp.concatenate(mats, 0)
    r = lax.broadcasted_iota(jnp.int32, both.shape, 0)
    c = lax.broadcasted_iota(jnp.int32, both.shape, 1) % width
    root = jnp.sum(jnp.where(r == c, both, 0.0), axis=0, keepdims=True)
    inv = lax.rsqrt(root * root)
    return both, jnp.where(c <= r, both * (inv * inv), 0.0)


def in_turns(steps, count):
    return [steps[len(steps) * g // count : len(steps) * (g + 1) // count] for g in range(count)]


def pair(x):
    return jnp.concatenate(split(x), 1)


def times(a, b):
    high, low = b
    k, n = high.shape
    right = jnp.concatenate(
        [jnp.concatenate([high, low], 1), jnp.concatenate([high, jnp.zeros_like(low)], 1)], 0
    )
    out = dot(a, right, NN)
    return out[:, :n] + out[:, n:]


def times_t(a, b):
    high, low = b
    n, k = high.shape
    right = jnp.concatenate(
        [jnp.concatenate([high, high], 1), jnp.concatenate([low, jnp.zeros_like(low)], 1)], 0
    )
    out = dot(a, right, NT)
    return out[:, :n] + out[:, n:]


def basis_of(beside, ucat_ref, basis_ref, tri_ref, a_ref, o_ref, y_ref, d_ref, l_ref, x_ref, p_ref, sems):
    n, inner = ucat_ref.shape
    blk = LANES
    nb = n // blk
    wide = 2 * blk
    groups = blk // SUB
    col = lax.axis_index("col")
    own = pl.ds(pl.multiple_of(col * blk, blk), blk)
    row_id = lax.broadcasted_iota(jnp.int32, (blk, blk), 0)
    col_id = lax.broadcasted_iota(jnp.int32, (blk, blk), 1)
    eye = row_id == col_id
    tiles = [(slice(r, r + wide), slice(c, c + wide)) for c in range(0, n, wide) for r in range(c, n, wide)]

    squares = jnp.zeros((SUB, inner), f32)
    for i in range(0, n, blk):
        top = ucat_ref[i : i + blk, :].astype(f32)
        squares = squares + jnp.sum((top * top).reshape(blk // SUB, SUB, inner), axis=0)
    shift = jnp.sum(squares) * (1.0 / (inner * n)) + 1e-06
    zero = jnp.zeros((SUB, LANES), f32) + shift * 0.0

    def diagonal(d, steps):
        d = d + jnp.where(eye, shift, 0.0)
        mats = [d[SUB * i : SUB * (i + 1), :] for i in range(groups)]
        turns = steps

        for g in eliminate([mats], groups, NEAR, LANES, zero):
            for step in turns[g]:
                step()
        both, inverse = factors_of(mats)
        return jnp.where(row_id <= col_id, both, 0.0).T, split(inverse)

    def spread(low, xs, b):
        nxt = jnp.minimum(b + 1, nb - 1)
        under = pl.ds(pl.multiple_of(nxt * blk, blk), blk)
        here = pl.ds(pl.multiple_of(b * blk, blk), blk)
        strip = a_ref[under, here]
        below = pair(times_t(pair(strip), xs))
        across = split(times_t(jnp.concatenate(xs, 1), split(strip)))
        d_ref[...] = a_ref[under, under] - times(below, across)
        l_ref[...] = low
        x_ref[0] = xs[0]
        x_ref[1] = xs[1]

    def copy_out(b):
        strip = pl.ds(pl.multiple_of(b * blk, blk), blk)
        return pltpu.make_async_copy(o_ref.at[b], tri_ref.at[0, :, strip], sems.at[b])

    y_ref[...] = ucat_ref[:, own].astype(f32)

    def gram(rows, cols):
        return dot(ucat_ref[rows, :], ucat_ref[cols, :], NT) * (1.0 / inner)

    def gram_step(rows, cols):
        a_ref[rows, cols] = gram(rows, cols)

    corner = slice(0, blk)
    turns = in_turns([functools.partial(gram_step, *t) for t in tiles], groups)
    for turn in turns:
        turn.append(lambda: next(beside, None))
    low, xs = diagonal(gram(corner, corner), turns)
    for _ in beside:
        pass
    spread(low, xs, 0)

    def block(b, carry):
        done = b - 1
        at = pl.ds(pl.multiple_of(done * blk, blk), blk)
        xs_old = (x_ref[0], x_ref[1])
        first = b * blk
        later = {}

        def solve_rows():
            yb = times(jnp.concatenate(xs_old, 1), split(y_ref[at, :]))
            basis_ref[0, at, :] = yb.astype(bf16)
            later["y"] = split(yb)

        def panel(r):
            rows = slice(r, r + wide)
            p = times_t(pair(a_ref[rows, at]), xs_old)
            ids = lax.broadcasted_iota(jnp.int32, (wide, blk), 0) + r
            p = jnp.where(ids >= first, p, 0.0)
            o_ref[done, rows, :] = p
            p_ref[rows, :] = pair(p)

        def trail(rows, cols):
            left = p_ref[rows, :]
            high, low = p_ref[cols, :blk], p_ref[cols, blk:]
            left = jnp.concatenate([left, left[:, :blk]], 1)
            a_ref[rows, cols] -= dot(left, jnp.concatenate([high, high, low], 1), NT)

        def rest(r):
            rows = slice(r, r + wide)
            y_ref[rows, :] -= times(p_ref[rows, :], later["y"])

        panels = [functools.partial(panel, r) for r in range(0, n, wide)]
        trails = [functools.partial(trail, *t) for t in tiles]
        rests = [functools.partial(rest, r) for r in range(0, n, wide)]
        steps = in_turns(panels, 2) + [[solve_rows]] + in_turns(trails + rests, groups - 3)
        low, xs = diagonal(d_ref[...], steps)
        o_ref[done, at, :] = l_ref[...]
        copy_out(done).start()
        spread(low, xs, b)
        return carry

    lax.fori_loop(1, nb, block, 0)
    last = slice(n - blk, n)
    o_ref[nb - 1, 0 : n - blk, :] = jnp.zeros((n - blk, blk), f32)
    o_ref[nb - 1, last, :] = l_ref[...]
    copy_out(nb - 1).start()
    xs = jnp.concatenate([x_ref[0], x_ref[1]], 1)
    basis_ref[0, last, :] = times(xs, split(y_ref[last, :])).astype(bf16)
    for b in range(nb):
        copy_out(b).wait()


def wave(a, b):
    dx, dy, dz = a[0] - b[0], a[1] - b[1], a[2] - b[2]
    square = dx * dx + dy * dy + dz * dz
    inverse = lax.rsqrt(square)
    turns = square * inverse * (WAVE_NUMBER / (2.0 * math.pi))
    x = 0.25 - jnp.abs(turns - lax.round(turns, lax.RoundingMethod.TO_NEAREST_EVEN))
    xx = x * x
    poly = SINE[-1]
    for c in SINE[-2::-1]:
        poly = poly * xx + c
    return (a[3] * b[3]) * (poly * x * inverse)


def apart(x, left):
    none = jnp.zeros_like(x)
    return jnp.concatenate([jnp.where(left, x, none), jnp.where(left, none, x)], 0)


def shifted_normals(tops):
    rank = tops[0].shape[0]
    groups = rank // SUB
    r = lax.broadcasted_iota(jnp.int32, tops[0].shape, 0)
    c = lax.broadcasted_iota(jnp.int32, tops[0].shape, 1)
    left = c < rank
    mats = []
    for top in tops:
        normal = times_t(pair(top), split(apart(top, left)))
        squares = jnp.sum(top * top, axis=0, keepdims=True)
        first = lax.broadcasted_iota(jnp.int32, squares.shape, 1) < rank
        shift = [jnp.sum(jnp.where(first == side, squares, 0.0), axis=1, keepdims=True) for side in (True, False)]
        shift = jnp.where(first, shift[0], shift[1]) * (1.0 / rank) + 1e-06
        normal = normal + jnp.where(r == c % rank, shift, 0.0)
        mats.append([normal[SUB * i : SUB * (i + 1), :] for i in range(groups)])
    return mats


def cross_blocks(rank, far_ref, tile_ref, ucat_ref, right_ref, pts_ref, ij_ref, ijt_ref, low_ref, half_ref, v_ref, panel_ref):
    devices = tile_ref.shape[0]
    cols = lax.axis_size("col")
    clusters = devices // cols
    size = cols * LANES
    local = far_ref.shape[1]
    slots = cols * local
    row, col = lax.axis_index("row"), lax.axis_index("col")
    left = lax.broadcasted_iota(jnp.int32, (rank, LANES), 1) < rank

    for k in range(clusters):
        p = jnp.concatenate([tile_ref[k * cols + c, 0:4, :] for c in range(cols)], 1)
        hi, mid = split(p)
        lo = (p - hi.astype(f32) - mid.astype(f32)).astype(bf16)
        zero = jnp.zeros((4, size), bf16)
        pts_ref[16 * k : 16 * k + 16, :] = jnp.concatenate([hi, mid, lo, zero], 0)

    spots = lax.broadcasted_iota(jnp.int32, (size, LANES), 0)
    of = lax.broadcasted_iota(jnp.int32, (clusters, 16, LANES), 0)
    for c in range(cols):
        for s in range(local):
            found = []
            for kind in range(2):
                panel = tile_ref[row * cols + c, 4 + kind * local + s : 5 + kind * local + s, :].astype(jnp.int32)
                where = panel // size
                hot = jnp.where(spots == panel - where * size, 1.0, 0.0).astype(bf16)
                got = dot(pts_ref[...], hot, NN).reshape(clusters, 16, LANES)
                got = jnp.sum(jnp.where(of == where[None], got, 0.0), axis=0)
                found.append(got[0:4] + got[4:8] + got[8:12])
            at = 8 * (c * local + s)
            ij_ref[at : at + 8, :] = jnp.concatenate(found, 0)
    ijt_ref[...] = jnp.concatenate([ij_ref[...], jnp.zeros((LANES - 8 * slots, LANES), f32)], 0).T

    def points_of(tile):
        both = jnp.concatenate([tile_ref[tile * cols + c, 0:4, :] for c in range(cols)], 1)
        return [both[i : i + 1, :] for i in range(4)]

    def columns(source, at, k):
        part = source[k * rank : (k + 1) * rank, :]
        return [jnp.broadcast_to(part[:, at + i : at + i + 1], (rank, LANES)) for i in range(4)]

    def both_rows(a, b, k):
        first = lax.broadcasted_iota(jnp.int32, (4, LANES), 1) < rank
        a, b = (b, a) if k else (a, b)
        other = pltpu.roll(b, rank, 1)
        got = jnp.where(first, other, a) if k else jnp.where(first, a, other)
        return [got[i : i + 1, :] for i in range(4)]

    def both_columns(a, b):
        return [jnp.where(left, x, y) for x, y in zip(a, b)]

    def against(column, points):
        wide = [jnp.concatenate([x] * cols, 1) for x in column]
        return wave(wide, points)

    own = points_of(row)

    pairs = []
    for s in range(0, slots, 2):
        rows_i = [ij_ref[8 * (s + h) : 8 * (s + h) + 4, :] for h in range(2)]
        j_cols = [[columns(ijt_ref, 8 * (s + h) + 4, k) for h in range(2)] for k in range(2)]
        i_rows = both_rows(rows_i[0], rows_i[1], 0)
        pairs.append([s, wave(both_columns(*j_cols[0]), i_rows), wave(both_columns(*j_cols[1]), i_rows), j_cols])

    mine = []
    for s in range(0, local, 2):
        which = (col * local + s) // 2
        rows = [ij_ref[pl.ds(pl.multiple_of(8 * (2 * which + h), 8), 8), :] for h in range(2)]
        flat = [r.T for r in rows]
        i_col = [[columns(flat[h], 0, k) for h in range(2)] for k in range(2)]
        j_col = [[columns(flat[h], 4, k) for h in range(2)] for k in range(2)]
        j_row = both_rows(rows[0][4:8], rows[1][4:8], 0)
        i_row = both_rows(rows[0][0:4], rows[1][0:4], 1)
        there = [points_of(far_ref[0, s + h]) for h in range(2)]
        mine.append((s, which, i_col, j_col, j_row, i_row, there))

    def left_factor(s, h, j_cols):
        at = (s + h) * 2 * rank
        ucat_ref[at : at + rank, :] = against(j_cols[0][h], own).astype(bf16)

    def row_panel(s, k, h, column, there):
        panel_ref[s // 2, k, h * rank : (h + 1) * rank, :] = against(column, there)

    def next_left_factor(s, j_cols):
        u0 = [ucat_ref[(s + h) * 2 * rank : (s + h) * 2 * rank + rank, :] for h in range(2)]
        product = dot(apart(v_ref[s // 2], left), jnp.concatenate(u0, 0), NN)
        for h in range(2):
            at = (s + h) * 2 * rank + rank
            u1 = against(j_cols[1][h], own) - product[h * rank : (h + 1) * rank]
            ucat_ref[at : at + rank, :] = u1.astype(bf16)

    fillers = [functools.partial(left_factor, p[0], h, p[3]) for p in pairs for h in range(2)]
    for s, _, i_col, _, _, _, there in mine:
        fillers += [
            functools.partial(row_panel, s, k, h, i_col[k][h], there[h]) for k in range(2) for h in range(2)
        ]
    groups = rank // SUB
    normals = shifted_normals([p[1] for p in pairs])
    turns = in_turns(fillers, groups)
    for g in eliminate(normals, groups, groups, rank):
        for step in turns[g]:
            step()
    lowers = [factors_of(rows, rank)[1] for rows in normals]
    for (s, top, mixed, _), low in zip(pairs, lowers):
        half = times(pair(low), split(apart(top, left)))
        low_ref[s // 2] = low
        half_ref[s // 2] = half
        v_t = times_t(pair(mixed), split(apart(half, left)))
        v_ref[s // 2] = times(pair(v_t), split(apart(low, left))).astype(bf16)

    for p in pairs:
        next_left_factor(p[0], p[3])

    square = lax.broadcasted_iota(jnp.int32, (LANES, LANES), 0) < rank
    same = square == (lax.broadcasted_iota(jnp.int32, (LANES, LANES), 1) < rank)

    def couple(low, half, panel):
        coupling = jnp.where(same, dot3(split(low), split(half), TN), 0.0)
        high, low = split(coupling)
        panel_high, panel_low = split(panel)
        both = jnp.concatenate([high, low], 1)
        return dot(both, jnp.concatenate([panel_high, panel_high], 0), NN) + dot(high, panel_low, NN)

    for s, which, i_col, j_col, j_row, i_row, there in mine:
        top = wave(both_columns(*j_col[1]), i_row)
        u_i = wave(both_columns(*j_col[0]), i_row).astype(bf16)
        top = top - dot(v_ref[which], apart(u_i, left), NN)
        normals = shifted_normals([top])
        v0 = couple(low_ref[which], half_ref[which], panel_ref[s // 2, 0]).astype(bf16)
        u_t = wave(both_columns(*i_col[1]), j_row).astype(bf16)
        rest = panel_ref[s // 2, 1] - dot(apart(u_t, left), v0, NN)
        zero = jnp.zeros((SUB, LANES), f32) + jnp.max(top) * 0.0
        yield from eliminate(normals, groups, groups, rank, zero)
        low = factors_of(normals[0], rank)[1]
        half = times(pair(low), split(apart(top, left)))
        yield groups
        v1 = couple(low, half, rest).astype(bf16)
        for h in range(2):
            at = (s + h) * 2 * rank
            right_ref[0, at : at + rank, :] = v0[h * rank : (h + 1) * rank]
            right_ref[0, at + rank : at + 2 * rank, :] = v1[h * rank : (h + 1) * rank]
        yield groups + 1


def main_kernel(rank, far_ref, tile_ref, right_ref, basis_ref, tri_ref, ucat_ref, *scratch):
    beside = cross_blocks(rank, far_ref, tile_ref, ucat_ref, right_ref, *scratch[:7])
    next(beside)
    basis_of(beside, ucat_ref, basis_ref, tri_ref, *scratch[7:])


def blocks_and_basis(far_blocks, tiles, rank, cols):
    local = far_blocks.shape[1]
    slots = cols * local
    clusters = tiles.shape[0] // cols
    size = cols * LANES
    n = slots * 2 * rank
    vmem = pl.BlockSpec(memory_space=pltpu.VMEM)
    return pl.pallas_call(
        functools.partial(main_kernel, rank),
        out_shape=(
            jax.ShapeDtypeStruct((1, local * 2 * rank, size), bf16),
            jax.ShapeDtypeStruct((1, n, LANES), bf16),
            jax.ShapeDtypeStruct((1, n, n), f32),
        ),
        in_specs=[pl.BlockSpec(memory_space=pltpu.SMEM), vmem],
        out_specs=(vmem, vmem, pl.BlockSpec(memory_space=pl.ANY)),
        scratch_shapes=[
            pltpu.VMEM((n, size), bf16),
            pltpu.VMEM((16 * clusters, size), bf16),
            pltpu.VMEM((8 * slots, LANES), f32),
            pltpu.VMEM((LANES, LANES), f32),
            pltpu.VMEM((slots // 2, rank, LANES), f32),
            pltpu.VMEM((slots // 2, rank, LANES), f32),
            pltpu.VMEM((slots // 2, rank, LANES), bf16),
            pltpu.VMEM((local // 2, 2, 2 * rank, size), f32),
            pltpu.VMEM((n, n), f32),
            pltpu.VMEM((n // LANES, n, LANES), f32),
            pltpu.VMEM((n, LANES), f32),
            pltpu.VMEM((LANES, LANES), f32),
            pltpu.VMEM((LANES, LANES), f32),
            pltpu.VMEM((2, LANES, LANES), bf16),
            pltpu.VMEM((n, 2 * LANES), bf16),
            pltpu.SemaphoreType.DMA((n // LANES,)),
        ],
        compiler_params=pltpu.CompilerParams(vmem_limit_bytes=48 << 20),
        name="blocks_and_basis",
    )(far_blocks, tiles)


def pack_kernel(size, far_ref, points_ref, weights_ref, row_ref, col_ref, out_ref):
    local = far_ref.shape[1]
    first = lax.axis_index("row") * size
    own = [row_ref[0, s] + first for s in range(local)]
    far = [col_ref[0, s] + far_ref[0, s] * size for s in range(local)]
    flat = [jnp.concatenate([x[k : k + 1] for k in range(x.shape[0])], 1).astype(f32) for x in own + far]
    tile = jnp.concatenate([points_ref[...], weights_ref[...]] + flat, 0)
    out_ref[...] = jnp.broadcast_to(tile[None], out_ref.shape)


def pack(far_blocks, points, weights, row_pivots, col_pivots, count, size):
    vmem = pl.BlockSpec(memory_space=pltpu.VMEM)
    return pl.pallas_call(
        functools.partial(pack_kernel, size),
        out_shape=jax.ShapeDtypeStruct((count, 4 + 2 * far_blocks.shape[1], points.shape[1]), f32),
        in_specs=[pl.BlockSpec(memory_space=pltpu.SMEM), vmem, vmem, vmem, vmem],
        out_specs=vmem,
        name="pack",
    )(far_blocks, points, weights[None], row_pivots, col_pivots)


def per_device(points, weights, far_blocks, row_pivots, col_pivots):
    part = points.shape[1]
    cols = lax.axis_size("col")
    rank = row_pivots.shape[3]
    count = lax.axis_size("row") * cols
    tiles = pack(far_blocks, points, weights, row_pivots, col_pivots, count, part * cols)
    tiles = lax.all_to_all(tiles, ("row", "col"), split_axis=0, concat_axis=0, tiled=True)
    factors_v, basis, lower = blocks_and_basis(far_blocks, tiles, rank, cols)
    return factors_v, basis, lower


def solution(mesh):
    return jax.shard_map(
        per_device,
        mesh=mesh,
        in_specs=(
            P(None, ("row", "col")),
            P(("row", "col")),
            P("row", "col"),
            P("row", "col", None, None),
            P("row", "col", None, None),
        ),
        out_specs=(P("row", "col", None), P("row", None, "col"), P("row", None, None)),
        check_vma=False,
    )
```

```python
import functools
import math

import jax
import jax.numpy as jnp
from jax import lax
from jax.experimental import pallas as pl
from jax.experimental.pallas import tpu as pltpu
from jax.sharding import PartitionSpec as P

f32, bf16 = jnp.float32, jnp.bfloat16
LANES, SUB = 128, 8

WAVE_NUMBER = 8.0
NEAR = 3
SINE = [6.283185273658022, -41.341677416633885, 81.60222657697675, -76.5748772418381, 39.71002372452099]
NN = (((1,), (0,)), ((), ()))
NT = (((1,), (1,)), ((), ()))
TN = (((0,), (0,)), ((), ()))


def dot(a, b, dims):
    return lax.dot_general(a, b, dims, preferred_element_type=f32)


def split(x):
    hi = x.astype(bf16)
    return hi, (x - hi.astype(f32)).astype(bf16)


def dot3(a, b, dims):
    ah, al = a if isinstance(a, tuple) else split(a)
    bh, bl = b if isinstance(b, tuple) else split(b)
    return dot(ah, bh, dims) + (dot(al, bh, dims) + dot(ah, bl, dims))


def row_bcast(x, j):
    return jnp.broadcast_to(x[j : j + 1, :], x.shape)


def eliminate(many, groups, near, width=LANES, zero=None):
    shape = many[0][0].shape
    sub = lax.broadcasted_iota(jnp.int32, shape, 0)
    lane = lax.broadcasted_iota(jnp.int32, shape, 1)
    start, spot = lane // width * width, lane % width
    look = zero is not None

    def lane_bcast(x, k):
        if width == LANES:
            return jnp.broadcast_to(x[:, k : k + 1], x.shape)
        return jnp.take_along_axis(x, start + k, axis=1, mode="promise_in_bounds")

    diagonals = [[lane_bcast(mats[0], t) + zero for t in range(SUB)] if look else None for mats in many]
    for g in range(groups):
        last = min(groups, g + near + 1)
        more = look and g + 1 < groups
        panels = [{} for _ in many]
        aheads = [{} for _ in many]
        for t in range(SUB):
            for mats, panel in zip(many, panels):
                for i in range(g + 1 if look else g, last):
                    panel[i, t] = lane_bcast(mats[i], SUB * g + t)
            for mats, ahead in zip(many, aheads):
                if more:
                    ahead[t] = lane_bcast(mats[g + 1], SUB * (g + 1) + t)
        for which, (mats, panel, ahead) in enumerate(zip(many, panels, aheads)):
            if look:
                diag = diagonals[which]
            else:
                diag = [panel[g, t] for t in range(SUB)]
            if more:
                panel[g + 1, 0] = panel[g + 1, 0] + zero
            rows, heads, scale = [], [], None
            for j in range(SUB):
                c = diag[j]
                root = lax.rsqrt(row_bcast(c, j))
                inv = root * root
                below = jnp.where(sub > j, c, 0.0)
                head = {}
                for t in range(j + 1, SUB):
                    raw = row_bcast(c, t)
                    head[t] = raw * inv
                    diag[t] = diag[t] - ((below * raw) * inv if t == j + 1 else below * head[t])
                row = row_bcast(mats[g], j) * jnp.where(spot == SUB * g + j, inv + inv, inv)
                mats[g] = mats[g] - below * row
                scale = root if j == 0 else jnp.where(sub == j, root, scale)
                rows.append(row)
                heads.append(head)
                if more:
                    c = panel[g + 1, j]
                    scaled = c * inv
                    for t in range(j + 1, SUB):
                        panel[g + 1, t] = panel[g + 1, t] - c * head[t]
                    for t in range(SUB):
                        ahead[t] = ahead[t] - scaled * row_bcast(c, t)
                    mats[g + 1] = mats[g + 1] - c * row
            mats[g] = mats[g] * scale
            if last < groups:
                inside = (spot >= SUB * g) & (spot < SUB * (g + 1))
                high, low = split(mats[g])
                right = jnp.where(inside & (spot > SUB * g + sub), 0.0, mats[g])
                right_high, right_low = split(right)
                none = jnp.zeros_like(high)
                product = dot(
                    jnp.concatenate([high, high, low, none], 0),
                    jnp.concatenate([right_high, right_low, right_high, none], 0),
                    TN,
                )
                for i in range(last, groups):
                    part = product[SUB * i : SUB * (i + 1), :]
                    for at in range(width, LANES, width):
                        part = jnp.where(lane < at, part, product[at + SUB * i : at + SUB * (i + 1), :])
                    mats[i] = jnp.where(inside, 0.0, mats[i]) - part
            for i in range(g + 2 if look else g + 1, last):
                for j in range(SUB):
                    for t in range(j + 1, SUB):
                        panel[i, t] = panel[i, t] - panel[i, j] * heads[j][t]
                    mats[i] = mats[i] - panel[i, j] * rows[j]
            diagonals[which] = ahead
        yield g


def factors_of(mats, width=LANES):
    both = jnp.concatenate(mats, 0)
    r = lax.broadcasted_iota(jnp.int32, both.shape, 0)
    c = lax.broadcasted_iota(jnp.int32, both.shape, 1) % width
    root = jnp.sum(jnp.where(r == c, both, 0.0), axis=0, keepdims=True)
    inv = lax.rsqrt(root * root)
    return both, jnp.where(c <= r, both * (inv * inv), 0.0)


def in_turns(steps, count):
    return [steps[len(steps) * g // count : len(steps) * (g + 1) // count] for g in range(count)]


def pair(x):
    return jnp.concatenate(split(x), 1)


def times(a, b):
    high, low = b
    k, n = high.shape
    right = jnp.concatenate(
        [jnp.concatenate([high, low], 1), jnp.concatenate([high, jnp.zeros_like(low)], 1)], 0
    )
    out = dot(a, right, NN)
    return out[:, :n] + out[:, n:]


def times_t(a, b):
    high, low = b
    n, k = high.shape
    right = jnp.concatenate(
        [jnp.concatenate([high, high], 1), jnp.concatenate([low, jnp.zeros_like(low)], 1)], 0
    )
    out = dot(a, right, NT)
    return out[:, :n] + out[:, n:]


def basis_of(beside, ucat_ref, basis_ref, tri_ref, a_ref, o_ref, y_ref, d_ref, l_ref, x_ref, p_ref, sems):
    n, inner = ucat_ref.shape
    blk = LANES
    nb = n // blk
    wide = 2 * blk
    groups = blk // SUB
    col = lax.axis_index("col")
    own = pl.ds(pl.multiple_of(col * blk, blk), blk)
    row_id = lax.broadcasted_iota(jnp.int32, (blk, blk), 0)
    col_id = lax.broadcasted_iota(jnp.int32, (blk, blk), 1)
    eye = row_id == col_id
    tiles = [(slice(r, r + wide), slice(c, c + wide)) for c in range(0, n, wide) for r in range(c, n, wide)]

    squares = jnp.zeros((SUB, inner), f32)
    for i in range(0, n, blk):
        top = ucat_ref[i : i + blk, :].astype(f32)
        squares = squares + jnp.sum((top * top).reshape(blk // SUB, SUB, inner), axis=0)
    shift = jnp.sum(squares) * (1.0 / (inner * n)) + 1e-06
    zero = jnp.zeros((SUB, LANES), f32) + shift * 0.0

    def diagonal(d, steps):
        d = d + jnp.where(eye, shift, 0.0)
        mats = [d[SUB * i : SUB * (i + 1), :] for i in range(groups)]
        turns = steps

        for g in eliminate([mats], groups, NEAR, LANES, zero):
            for step in turns[g]:
                step()
        both, inverse = factors_of(mats)
        return jnp.where(row_id <= col_id, both, 0.0).T, split(inverse)

    def spread(low, xs, b):
        nxt = jnp.minimum(b + 1, nb - 1)
        under = pl.ds(pl.multiple_of(nxt * blk, blk), blk)
        here = pl.ds(pl.multiple_of(b * blk, blk), blk)
        strip = a_ref[under, here]
        below = pair(times_t(pair(strip), xs))
        across = split(times_t(jnp.concatenate(xs, 1), split(strip)))
        d_ref[...] = a_ref[under, under] - times(below, across)
        l_ref[...] = low
        x_ref[0] = xs[0]
        x_ref[1] = xs[1]

    def copy_out(b):
        strip = pl.ds(pl.multiple_of(b * blk, blk), blk)
        return pltpu.make_async_copy(o_ref.at[b], tri_ref.at[0, :, strip], sems.at[b])

    y_ref[...] = ucat_ref[:, own].astype(f32)

    def gram(rows, cols):
        return dot(ucat_ref[rows, :], ucat_ref[cols, :], NT) * (1.0 / inner)

    def gram_step(rows, cols):
        a_ref[rows, cols] = gram(rows, cols)

    corner = slice(0, blk)
    turns = in_turns([functools.partial(gram_step, *t) for t in tiles], groups)
    for turn in turns:
        turn.append(lambda: next(beside, None))
    low, xs = diagonal(gram(corner, corner), turns)
    for _ in beside:
        pass
    spread(low, xs, 0)

    def block(b, carry):
        done = b - 1
        at = pl.ds(pl.multiple_of(done * blk, blk), blk)
        xs_old = (x_ref[0], x_ref[1])
        first = b * blk
        later = {}

        def solve_rows():
            yb = times(jnp.concatenate(xs_old, 1), split(y_ref[at, :]))
            basis_ref[0, at, :] = yb.astype(bf16)
            later["y"] = split(yb)

        def panel(r):
            rows = slice(r, r + wide)
            p = times_t(pair(a_ref[rows, at]), xs_old)
            ids = lax.broadcasted_iota(jnp.int32, (wide, blk), 0) + r
            p = jnp.where(ids >= first, p, 0.0)
            o_ref[done, rows, :] = p
            p_ref[rows, :] = pair(p)

        def trail(rows, cols):
            left = p_ref[rows, :]
            high, low = p_ref[cols, :blk], p_ref[cols, blk:]
            left = jnp.concatenate([left, left[:, :blk]], 1)
            a_ref[rows, cols] -= dot(left, jnp.concatenate([high, high, low], 1), NT)

        def rest(r):
            rows = slice(r, r + wide)
            y_ref[rows, :] -= times(p_ref[rows, :], later["y"])

        panels = [functools.partial(panel, r) for r in range(0, n, wide)]
        trails = [functools.partial(trail, *t) for t in tiles]
        rests = [functools.partial(rest, r) for r in range(0, n, wide)]
        steps = in_turns(panels, 2) + [[solve_rows]] + in_turns(trails + rests, groups - 3)
        low, xs = diagonal(d_ref[...], steps)
        o_ref[done, at, :] = l_ref[...]
        copy_out(done).start()
        spread(low, xs, b)
        return carry

    lax.fori_loop(1, nb, block, 0)
    last = slice(n - blk, n)
    o_ref[nb - 1, 0 : n - blk, :] = jnp.zeros((n - blk, blk), f32)
    o_ref[nb - 1, last, :] = l_ref[...]
    copy_out(nb - 1).start()
    xs = jnp.concatenate([x_ref[0], x_ref[1]], 1)
    basis_ref[0, last, :] = times(xs, split(y_ref[last, :])).astype(bf16)
    for b in range(nb):
        copy_out(b).wait()


def wave(a, b):
    dx, dy, dz = a[0] - b[0], a[1] - b[1], a[2] - b[2]
    square = dx * dx + dy * dy + dz * dz
    inverse = lax.rsqrt(square)
    turns = square * inverse * (WAVE_NUMBER / (2.0 * math.pi))
    x = 0.25 - jnp.abs(turns - lax.round(turns, lax.RoundingMethod.TO_NEAREST_EVEN))
    xx = x * x
    poly = SINE[-1]
    for c in SINE[-2::-1]:
        poly = poly * xx + c
    return (a[3] * b[3]) * (poly * x * inverse)


def apart(x, left):
    none = jnp.zeros_like(x)
    return jnp.concatenate([jnp.where(left, x, none), jnp.where(left, none, x)], 0)


def shifted_normals(tops):
    rank = tops[0].shape[0]
    groups = rank // SUB
    r = lax.broadcasted_iota(jnp.int32, tops[0].shape, 0)
    c = lax.broadcasted_iota(jnp.int32, tops[0].shape, 1)
    left = c < rank
    mats = []
    for top in tops:
        normal = times_t(pair(top), split(apart(top, left)))
        squares = jnp.sum(top * top, axis=0, keepdims=True)
        first = lax.broadcasted_iota(jnp.int32, squares.shape, 1) < rank
        shift = [jnp.sum(jnp.where(first == side, squares, 0.0), axis=1, keepdims=True) for side in (True, False)]
        shift = jnp.where(first, shift[0], shift[1]) * (1.0 / rank) + 1e-06
        normal = normal + jnp.where(r == c % rank, shift, 0.0)
        mats.append([normal[SUB * i : SUB * (i + 1), :] for i in range(groups)])
    return mats


def cross_blocks(rank, far_ref, tile_ref, ucat_ref, right_ref, pts_ref, ij_ref, ijt_ref, low_ref, half_ref, v_ref, panel_ref):
    devices = tile_ref.shape[0]
    cols = lax.axis_size("col")
    clusters = devices // cols
    size = cols * LANES
    local = far_ref.shape[1]
    slots = cols * local
    row, col = lax.axis_index("row"), lax.axis_index("col")
    left = lax.broadcasted_iota(jnp.int32, (rank, LANES), 1) < rank

    for k in range(clusters):
        p = jnp.concatenate([tile_ref[k * cols + c, 0:4, :] for c in range(cols)], 1)
        hi, mid = split(p)
        lo = (p - hi.astype(f32) - mid.astype(f32)).astype(bf16)
        zero = jnp.zeros((4, size), bf16)
        pts_ref[16 * k : 16 * k + 16, :] = jnp.concatenate([hi, mid, lo, zero], 0)

    spots = lax.broadcasted_iota(jnp.int32, (size, LANES), 0)
    of = lax.broadcasted_iota(jnp.int32, (clusters, 16, LANES), 0)
    for c in range(cols):
        for s in range(local):
            found = []
            for kind in range(2):
                panel = tile_ref[row * cols + c, 4 + kind * local + s : 5 + kind * local + s, :].astype(jnp.int32)
                where = panel // size
                hot = jnp.where(spots == panel - where * size, 1.0, 0.0).astype(bf16)
                if kind == 0:
                    got = dot(pts_ref[pl.ds(pl.multiple_of(16 * row, 16), 16), :], hot, NN)
                else:
                    got = dot(pts_ref[...], hot, NN).reshape(clusters, 16, LANES)
                    got = jnp.sum(jnp.where(of == where[None], got, 0.0), axis=0)
                found.append(got[0:4] + got[4:8] + got[8:12])
            at = 8 * (c * local + s)
            ij_ref[at : at + 8, :] = jnp.concatenate(found, 0)
    ijt_ref[...] = jnp.concatenate([ij_ref[...], jnp.zeros((LANES - 8 * slots, LANES), f32)], 0).T

    def points_of(tile):
        both = jnp.concatenate([tile_ref[tile * cols + c, 0:4, :] for c in range(cols)], 1)
        return [both[i : i + 1, :] for i in range(4)]

    def columns(source, at, k):
        part = source[k * rank : (k + 1) * rank, :]
        return [jnp.broadcast_to(part[:, at + i : at + i + 1], (rank, LANES)) for i in range(4)]

    def both_rows(a, b, k):
        first = lax.broadcasted_iota(jnp.int32, (4, LANES), 1) < rank
        a, b = (b, a) if k else (a, b)
        other = pltpu.roll(b, rank, 1)
        got = jnp.where(first, other, a) if k else jnp.where(first, a, other)
        return [got[i : i + 1, :] for i in range(4)]

    def both_columns(a, b):
        return [jnp.where(left, x, y) for x, y in zip(a, b)]

    def against(column, points):
        wide = [jnp.concatenate([x] * cols, 1) for x in column]
        return wave(wide, points)

    own = points_of(row)

    pairs = []
    for s in range(0, slots, 2):
        rows_i = [ij_ref[8 * (s + h) : 8 * (s + h) + 4, :] for h in range(2)]
        j_cols = [[columns(ijt_ref, 8 * (s + h) + 4, k) for h in range(2)] for k in range(2)]
        i_rows = both_rows(rows_i[0], rows_i[1], 0)
        pairs.append([s, wave(both_columns(*j_cols[0]), i_rows), wave(both_columns(*j_cols[1]), i_rows), j_cols])

    mine = []
    for s in range(0, local, 2):
        which = (col * local + s) // 2
        rows = [ij_ref[pl.ds(pl.multiple_of(8 * (2 * which + h), 8), 8), :] for h in range(2)]
        flat = [r.T for r in rows]
        i_col = [[columns(flat[h], 0, k) for h in range(2)] for k in range(2)]
        j_col = [[columns(flat[h], 4, k) for h in range(2)] for k in range(2)]
        j_row = both_rows(rows[0][4:8], rows[1][4:8], 0)
        i_row = both_rows(rows[0][0:4], rows[1][0:4], 1)
        there = [points_of(far_ref[0, s + h]) for h in range(2)]
        mine.append((s, which, i_col, j_col, j_row, i_row, there))

    def left_factor(s, h, j_cols):
        at = (s + h) * 2 * rank
        ucat_ref[at : at + rank, :] = against(j_cols[0][h], own).astype(bf16)

    def row_panel(s, k, h, column, there):
        panel_ref[s // 2, k, h * rank : (h + 1) * rank, :] = against(column, there)

    def next_left_factor(s, j_cols):
        u0 = [ucat_ref[(s + h) * 2 * rank : (s + h) * 2 * rank + rank, :] for h in range(2)]
        product = dot(apart(v_ref[s // 2], left), jnp.concatenate(u0, 0), NN)
        for h in range(2):
            at = (s + h) * 2 * rank + rank
            u1 = against(j_cols[1][h], own) - product[h * rank : (h + 1) * rank]
            ucat_ref[at : at + rank, :] = u1.astype(bf16)

    fillers = [functools.partial(left_factor, p[0], h, p[3]) for p in pairs for h in range(2)]
    for s, _, i_col, _, _, _, there in mine:
        fillers += [
            functools.partial(row_panel, s, k, h, i_col[k][h], there[h]) for k in range(2) for h in range(2)
        ]
    groups = rank // SUB
    normals = shifted_normals([p[1] for p in pairs])
    turns = in_turns(fillers, groups)
    for g in eliminate(normals, groups, groups, rank):
        for step in turns[g]:
            step()
    lowers = [factors_of(rows, rank)[1] for rows in normals]
    for (s, top, mixed, _), low in zip(pairs, lowers):
        half = times(pair(low), split(apart(top, left)))
        low_ref[s // 2] = low
        half_ref[s // 2] = half
        v_t = times_t(pair(mixed), split(apart(half, left)))
        v_ref[s // 2] = times(pair(v_t), split(apart(low, left))).astype(bf16)

    for p in pairs:
        next_left_factor(p[0], p[3])

    square = lax.broadcasted_iota(jnp.int32, (LANES, LANES), 0) < rank
    same = square == (lax.broadcasted_iota(jnp.int32, (LANES, LANES), 1) < rank)

    def couple(low, half, panel):
        coupling = jnp.where(same, dot3(split(low), split(half), TN), 0.0)
        high, low = split(coupling)
        panel_high, panel_low = split(panel)
        both = jnp.concatenate([high, low], 1)
        return dot(both, jnp.concatenate([panel_high, panel_high], 0), NN) + dot(high, panel_low, NN)

    for s, which, i_col, j_col, j_row, i_row, there in mine:
        top = wave(both_columns(*j_col[1]), i_row)
        u_i = wave(both_columns(*j_col[0]), i_row).astype(bf16)
        top = top - dot(v_ref[which], apart(u_i, left), NN)
        normals = shifted_normals([top])
        v0 = couple(low_ref[which], half_ref[which], panel_ref[s // 2, 0]).astype(bf16)
        u_t = wave(both_columns(*i_col[1]), j_row).astype(bf16)
        rest = panel_ref[s // 2, 1] - dot(apart(u_t, left), v0, NN)
        zero = jnp.zeros((SUB, LANES), f32) + jnp.max(top) * 0.0
        yield from eliminate(normals, groups, groups, rank, zero)
        low = factors_of(normals[0], rank)[1]
        half = times(pair(low), split(apart(top, left)))
        yield groups
        v1 = couple(low, half, rest).astype(bf16)
        for h in range(2):
            at = (s + h) * 2 * rank
            right_ref[0, at : at + rank, :] = v0[h * rank : (h + 1) * rank]
            right_ref[0, at + rank : at + 2 * rank, :] = v1[h * rank : (h + 1) * rank]
        yield groups + 1


def main_kernel(rank, far_ref, tile_ref, right_ref, basis_ref, tri_ref, ucat_ref, *scratch):
    beside = cross_blocks(rank, far_ref, tile_ref, ucat_ref, right_ref, *scratch[:7])
    next(beside)
    basis_of(beside, ucat_ref, basis_ref, tri_ref, *scratch[7:])


def blocks_and_basis(far_blocks, tiles, rank, cols):
    local = far_blocks.shape[1]
    slots = cols * local
    clusters = tiles.shape[0] // cols
    size = cols * LANES
    n = slots * 2 * rank
    vmem = pl.BlockSpec(memory_space=pltpu.VMEM)
    return pl.pallas_call(
        functools.partial(main_kernel, rank),
        out_shape=(
            jax.ShapeDtypeStruct((1, local * 2 * rank, size), bf16),
            jax.ShapeDtypeStruct((1, n, LANES), bf16),
            jax.ShapeDtypeStruct((1, n, n), f32),
        ),
        in_specs=[pl.BlockSpec(memory_space=pltpu.SMEM), vmem],
        out_specs=(vmem, vmem, pl.BlockSpec(memory_space=pl.ANY)),
        scratch_shapes=[
            pltpu.VMEM((n, size), bf16),
            pltpu.VMEM((16 * clusters, size), bf16),
            pltpu.VMEM((8 * slots, LANES), f32),
            pltpu.VMEM((LANES, LANES), f32),
            pltpu.VMEM((slots // 2, rank, LANES), f32),
            pltpu.VMEM((slots // 2, rank, LANES), f32),
            pltpu.VMEM((slots // 2, rank, LANES), bf16),
            pltpu.VMEM((local // 2, 2, 2 * rank, size), f32),
            pltpu.VMEM((n, n), f32),
            pltpu.VMEM((n // LANES, n, LANES), f32),
            pltpu.VMEM((n, LANES), f32),
            pltpu.VMEM((LANES, LANES), f32),
            pltpu.VMEM((LANES, LANES), f32),
            pltpu.VMEM((2, LANES, LANES), bf16),
            pltpu.VMEM((n, 2 * LANES), bf16),
            pltpu.SemaphoreType.DMA((n // LANES,)),
        ],
        compiler_params=pltpu.CompilerParams(vmem_limit_bytes=48 << 20),
        name="blocks_and_basis",
    )(far_blocks, tiles)


def pack_kernel(size, far_ref, points_ref, weights_ref, row_ref, col_ref, out_ref):
    local = far_ref.shape[1]
    first = lax.axis_index("row") * size
    own = [row_ref[0, s] + first for s in range(local)]
    far = [col_ref[0, s] + far_ref[0, s] * size for s in range(local)]
    flat = [jnp.concatenate([x[k : k + 1] for k in range(x.shape[0])], 1).astype(f32) for x in own + far]
    tile = jnp.concatenate([points_ref[...], weights_ref[...]] + flat, 0)
    out_ref[...] = jnp.broadcast_to(tile[None], out_ref.shape)


def pack(far_blocks, points, weights, row_pivots, col_pivots, count, size):
    vmem = pl.BlockSpec(memory_space=pltpu.VMEM)
    return pl.pallas_call(
        functools.partial(pack_kernel, size),
        out_shape=jax.ShapeDtypeStruct((count, 4 + 2 * far_blocks.shape[1], points.shape[1]), f32),
        in_specs=[pl.BlockSpec(memory_space=pltpu.SMEM), vmem, vmem, vmem, vmem],
        out_specs=vmem,
        name="pack",
    )(far_blocks, points, weights[None], row_pivots, col_pivots)


def per_device(points, weights, far_blocks, row_pivots, col_pivots):
    part = points.shape[1]
    cols = lax.axis_size("col")
    rank = row_pivots.shape[3]
    count = lax.axis_size("row") * cols
    tiles = pack(far_blocks, points, weights, row_pivots, col_pivots, count, part * cols)
    tiles = lax.all_to_all(tiles, ("row", "col"), split_axis=0, concat_axis=0, tiled=True)
    factors_v, basis, lower = blocks_and_basis(far_blocks, tiles, rank, cols)
    return factors_v, basis, lower


def solution(mesh):
    return jax.shard_map(
        per_device,
        mesh=mesh,
        in_specs=(
            P(None, ("row", "col")),
            P(("row", "col")),
            P("row", "col"),
            P("row", "col", None, None),
            P("row", "col", None, None),
        ),
        out_specs=(P("row", "col", None), P("row", None, "col"), P("row", None, None)),
        check_vma=False,
    )
```
